32 devices in a mesh: frag: 2 (over y), band: 8 (over z, x), slab: 2 (over core).
Axes of the slice: x: 2, y: 2, z: 4, core: 2. Of those that a mesh axis runs over, the one named last changes fastest.
Arguments:
- wavefunctions: bfloat16 [2048, 16384], P('band', ('frag', 'slab')), parts along dimension 1, may hold values from -6 to 6
- eigvec: bfloat16 [2048, 4096], P(None, ('frag', 'band', 'slab')), parts along dimension 1, may hold values from -1 to 1, as said below
- occupation: float32 [4096], P('frag'), parts along dimension 0, may hold values from 0.1 to 2
Outputs:
- rotated: float32 [2048, 16384], P('band', ('frag', 'slab')), parts along dimension 1
- density: float32 [16384], P(('frag', 'slab')), parts along dimension 0
The draws below stay inside these ranges and needn't reach their ends.
There are 2 independent parts, one for each index of `frag`. The reference program is written for one: setup_inputs(seed, part) draws one part's arguments, and reference() takes and returns one part's arrays. A program takes and returns all parts, laid end to end along the dimension named above; each array names one. Nothing has to cross between parts.
Inputs may be any that keep to these rules, and one draw needn't show every extreme that they name: eigvec is an orthogonal matrix rounded to bfloat16.
All inputs are finite; a program needn't handle non-finite values.
Results may differ from the reference program's by a relative error of at most 0.0003.
Values may be sent and summed in bfloat16 or wider, within the bound.
A program may use at most 64 MiB of HBM per device.

```python
import math
import jax
import jax.numpy as jnp

NB = 2048
NPTS = 8192


def draw_eigvec(key, part):
    sample = jax.random.normal(jax.random.fold_in(key, 7), (NB, NB), jnp.float32)
    basis, upper = jnp.linalg.qr(sample)
    signs = jnp.where(jnp.diagonal(upper) < 0, -1.0, 1.0).astype(jnp.float32)
    return (basis * signs[None, :]).astype(jnp.bfloat16)


def level_of(rng, shape, pieces, low, largest):
    loudness = 1.0
    for dim, shards_of in pieces:
        draws = jax.random.uniform(jax.random.fold_in(jax.random.fold_in(rng, 6), dim), (shards_of,), jnp.float32, low / len(pieces), largest / len(pieces))
        loudness = loudness * jnp.repeat(jnp.exp(draws), shape[dim] // shards_of).reshape((-1,) + (1,) * (len(shape) - 1 - dim))
    return loudness


def normal_values(rng, dims, deviation, limit, cuts=(), held_as=jnp.bfloat16):
    values = deviation * jax.random.normal(rng, dims, jnp.float32)
    if cuts:
        values = values * level_of(rng, dims, cuts, -0.22, 0.18)
    return jnp.clip(values, -limit, limit).astype(held_as)


def setup_inputs(seed: int = 0, part: int = 0) -> dict:
    arg_keys = jax.random.split(jax.random.key(seed), 4)
    part_keys = jax.random.split(jax.random.fold_in(arg_keys[3], part), 4)
    return {
        "wavefunctions": normal_values(part_keys[0], (NB, NPTS), 1.0, 6.0, ((0, 8), (1, 2))),
        "eigvec": draw_eigvec(jax.random.fold_in(jax.random.fold_in(arg_keys[3], part), 71), part),
        "occupation": jnp.clip(jnp.exp(jax.random.uniform(part_keys[2], (NB,), jnp.float32, math.log(0.1), math.log(2.0))), 0.1, 2.0),
    }


def reference(wavefunctions, eigvec, occupation):
    rotated = jnp.dot(eigvec.T.astype(jnp.float32), wavefunctions.astype(jnp.float32), preferred_element_type=jnp.float32)
    weighted = occupation[:, None] * rotated * rotated
    density = jnp.sum(weighted, axis=0) / jnp.float32(NB)
    return (rotated, density)
```

```python
import functools

import jax
import jax.numpy as jnp
from jax import lax
from jax.experimental import pallas as pl
from jax.experimental.pallas import tpu as pltpu
from jax.sharding import PartitionSpec as P

MESH = pl.DeviceIdType.MESH
LANES = 128
SHARED = 2


def plain(wavefunctions, eigvec, occupation):
    total_bands = eigvec.shape[0]
    by_points = lax.all_to_all(wavefunctions, "band", split_axis=1, concat_axis=0, tiled=True)
    point_rows = lax.dot_general(
        lax.all_gather(eigvec, ("band", "slab"), axis=1, tiled=True),
        by_points,
        (((0,), (0,)), ((), ())),
        preferred_element_type=jnp.float32,
    )
    rotated = lax.all_to_all(point_rows, "band", split_axis=0, concat_axis=1, tiled=True)
    local_density = jnp.dot(
        occupation,
        point_rows * point_rows,
        precision=lax.Precision.HIGHEST,
        preferred_element_type=jnp.float32,
    ) / jnp.float32(total_bands)
    density = lax.all_gather(local_density, "band", axis=0, tiled=True)
    return (rotated, density)


def kernel(
    wave, eigvec, occupation, out, density,
    gathered, away, raw, vectors, seats, weight, staged, passing, part, parts,
    own_in, away_in, raw_in, seats_in, arrive, away_out, peer_out, mate_out, share_out,
    vec_in, vec_core, vec_side, vec_mate, res_mate, pass_in, mate_in, side_in, side_out, part_out, part_in,
):
    nb, nz = gathered.shape[1], gathered.shape[1] // 2
    frag, band, slab = (lax.axis_index(name) for name in ("frag", "band", "slab"))
    z, x = band // 2, lax.rem(band, 2)
    end = z // 2
    inner = (z == 1) | (z == 2)
    outer = (z == 0) | (z == 3)
    rows, points = wave.shape
    half = points // 2
    steps = half // LANES
    total_bands, width = eigvec.shape
    deep = total_bands // nz
    tall = rows // 2
    ahead = SHARED

    mate_z = 4 * end + 1 - z
    beside = band + 1 - 2 * x
    mate, mate_beside = 2 * mate_z + x, 2 * mate_z + 1 - x
    peer, peer_beside = 2 * (3 - z) + x, 2 * (3 - z) + 1 - x
    far, far_beside = 2 * (3 - mate_z) + x, 2 * (3 - mate_z) + 1 - x

    def at(b, s=slab):
        return (frag, b, s)

    def send(src, dst, ssem, rsem, target):
        return pltpu.make_async_remote_copy(
            src_ref=src, dst_ref=dst, send_sem=ssem, recv_sem=rsem, device_id=target, device_id_type=MESH
        )

    def columns(of, step):
        return pl.ds(pl.multiple_of(of * half + step * LANES, LANES), LANES)

    def own_load(step):
        return pltpu.make_async_copy(wave.at[:, columns(x, step)], gathered.at[step, band], own_in.at[step])

    def away_load(step):
        return pltpu.make_async_copy(wave.at[:, columns(1 - x, step)], away.at[step], away_in.at[step])

    def raw_load(q):
        piece = pl.ds(q * deep, deep)
        return pltpu.make_async_copy(eigvec.at[piece], raw.at[piece], raw_in.at[q])

    seats_load = pltpu.make_async_copy(occupation, seats, seats_in.at[0])

    def across(step):
        return send(away.at[step], gathered.at[step, band], away_out.at[step], arrive.at[step, band], at(beside))

    def block(step, b, sem, target):
        there = gathered.at[step, b]
        return send(there, there, sem, arrive.at[step, b], at(target))

    def arrived(step, b):
        block(step, b, away_out.at[step], beside).wait_recv()

    def seat_of(b):
        return b - 4 * end

    def panel(b, s, q, sem, target):
        seat = seat_of(b) * 2 + s
        there = vectors.at[q, pl.ds(pl.multiple_of(seat * width, width), width)]
        return send(there, there, sem, vec_in.at[seat, q], target)

    def to_core(which, b, q):
        return panel(b, slab, q, vec_core.at[which, q], at(band, 1 - slab))

    def to_side(which, b, q):
        return panel(b, slab, q, vec_side.at[which, q], at(beside))

    def to_mate(q):
        return panel(band, slab, q, vec_mate.at[q], at(mate))

    def panel_wait(b, s, q):
        panel(b, s, q, vec_core.at[0, q], at(beside)).wait_recv()

    def tile(p):
        return pl.ds(p * tall, tall)

    def to_pass(step, p):
        return send(staged.at[step, 0, tile(p)], passing.at[step, tile(p)], res_mate.at[step, p], pass_in.at[step, p], at(mate))

    def to_mate_out(step, p):
        there = out.at[tile(p), columns(x, step)]
        return send(staged.at[step, 1, tile(p)], there, res_mate.at[step, 2 + p], mate_in.at[step, p], at(mate))

    def to_side_out(src, step, p):
        return send(src, out.at[tile(p), columns(x, step)], side_out.at[step, p], side_in.at[step, p], at(beside))

    def from_side_out(step, p):
        there = out.at[tile(p), columns(1 - x, step)]
        send(there, there, side_out.at[step, p], side_in.at[step, p], at(beside)).wait_recv()

    def product(step, b):
        first = pl.multiple_of(seat_of(b) * rows, rows)
        total = None
        for q in range(nz):
            term = jnp.dot(
                vectors[q, pl.ds(first, rows), :],
                gathered[step, pl.ds(2 * q, 2)].reshape(deep, LANES),
                preferred_element_type=jnp.float32,
            )
            total = term if total is None else total + term
        part[step] = part[step] + jnp.sum(weight[pl.ds(first, rows), :] * total * total, axis=0, keepdims=True)
        return total

    def load(step, carry):
        away_load(step).start()
        own_load(step).start()
        return carry

    lax.fori_loop(0, 4, load, 0)
    for q in range(nz):
        raw_load(q).start()
    lax.fori_loop(4, steps, load, 0)
    seats_load.start()

    barrier = pltpu.get_barrier_semaphore()
    for target in (at(beside), at(mate), at(band, 1 - slab)):
        pl.semaphore_signal(barrier, inc=1, device_id=target, device_id_type=MESH)

    @pl.when(inner)
    def _():
        pl.semaphore_signal(barrier, inc=1, device_id=at(peer), device_id_type=MESH)
        pl.semaphore_wait(barrier, 4)

    @pl.when(outer)
    def _():
        pl.semaphore_wait(barrier, 3)

    def exchange(step):
        away_load(step).wait()
        across(step).start()

    def turn():
        for q in range(nz):
            raw_load(q).wait()
            first = pl.multiple_of((seat_of(band) * 2 + slab) * width, width)
            vectors[q, pl.ds(first, width), :] = raw[pl.ds(q * deep, deep), :].T

    def weigh():
        seats_load.wait()
        for group in range(8):
            row = seats[pl.ds(pl.multiple_of(8 * end, 8), 8), :][group : group + 1, :]
            weight[pl.ds(group * LANES, LANES), :] = jnp.broadcast_to(row, (LANES, LANES)).T

    part[...] = jnp.zeros(part.shape, part.dtype)

    @pl.when(inner)
    def _():
        def onward(step, b, i):
            block(step, b, peer_out.at[step, i], peer).start()

        def share(step, b, i):
            block(step, b, share_out.at[step, i], mate).start()

        def mine(step, shared=False):
            own_load(step).wait()
            onward(step, band, 0)
            if shared:
                share(step, band, 0)

        def side(step, shared=False):
            arrived(step, beside)
            onward(step, beside, 1)
            if shared:
                share(step, beside, 1)

        def mates(step):
            for i, b in ((2, mate), (3, mate_beside)):
                arrived(step, b)
                onward(step, b, i)

        def fars(step, shared=False):
            for i, b in ((2, peer), (3, peer_beside), (4, far), (5, far_beside)):
                arrived(step, b)
                if shared:
                    share(step, b, i)

        mine(0, True)
        exchange(0)
        mine(1, True)
        exchange(1)
        exchange(2)
        turn()
        for q in range(nz):
            to_core(0, band, q).start()
        for q in range(2):
            to_side(0, band, q).start()
        weigh()
        for step in range(ahead + 1):
            if step > 1:
                mine(step, step < ahead)
            side(step, step < ahead)
            mates(step)
            if 0 < step:
                fars(step - 1, True)
        exchange(3)
        mine(ahead + 1)
        side(ahead + 1)
        exchange(4)
        for q in range(nz):
            panel_wait(mate, slab, q)
            to_side(1, mate, q).start()
            to_core(2, mate, q).start()
            if q == 1:
                mine(ahead + 2)
                side(ahead + 2)
                exchange(5)
        mine(ahead + 3)
        side(ahead + 3)
        exchange(6)
        for q in range(2, nz):
            to_side(0, band, q).start()
        for q in range(nz):
            panel_wait(mate_beside, slab, q)
            to_core(3, mate_beside, q).start()

        def for_mate(step):
            staged[step, 0] = product(step, mate_beside)
            for p in range(2):
                to_pass(step, p).start()
            staged[step, 1] = product(step, mate)
            for p in range(2):
                to_mate_out(step, p).start()

        def for_row(step):
            staged[step, 2] = product(step, beside)
            for p in range(2):
                to_side_out(staged.at[step, 2, tile(p)], step, p).start()
            out[:, columns(x, step)] = product(step, band)

        def body(step, carry):
            @pl.when(step + 1 < steps)
            def _():
                mates(step + 1)

            @pl.when((step >= ahead + 2) & (step + 2 < steps))
            def _():
                mine(step + 2)
                side(step + 2)

            @pl.when(step + 5 < steps)
            def _():
                exchange(step + 5)

            fars(step)

            @pl.when(step == ahead)
            def _():
                for q in range(nz):
                    panel_wait(mate, 1 - slab, q)
                    panel_wait(mate_beside, 1 - slab, q)

            for_mate(step)

            @pl.when(step == ahead)
            def _():
                for q in range(nz):
                    panel_wait(beside, slab, q)
                    to_core(1, beside, q).start()
                for q in range(nz):
                    panel_wait(band, 1 - slab, q)
                    panel_wait(beside, 1 - slab, q)

            for_row(step - ahead)
            return carry

        lax.fori_loop(ahead, steps, body, 0)

        def rest(step, carry):
            for_row(step)
            return carry

        lax.fori_loop(steps - ahead, steps, rest, 0)

    @pl.when(outer)
    def _():
        def up(step, b, i):
            return block(step, b, mate_out.at[step, i], mate)

        def mine(step):
            own_load(step).wait()
            up(step, band, 0).start()

        def side(step):
            arrived(step, beside)
            up(step, beside, 1).start()

        for step in range(ahead + 1):
            exchange(step)
            mine(step)
        turn()
        for step in range(ahead + 1):
            side(step)
        for q in range(nz):
            to_mate(q).start()
        for step in range(ahead + 1, ahead + 6):
            exchange(step)
        for q in range(nz):
            to_side(0, band, q).start()
            to_core(0, band, q).start()

        def begin(step, carry):
            exchange(step)
            return carry

        lax.fori_loop(ahead + 6, steps, begin, 0)
        weigh()
        for step in range(ahead + 1, ahead + 6):
            mine(step)
            side(step)
        for q in range(nz):
            panel_wait(beside, slab, q)
            to_core(1, beside, q).start()
        for q in range(nz):
            panel_wait(band, 1 - slab, q)
            panel_wait(beside, 1 - slab, q)
        for step in range(ahead):
            for b in (mate, mate_beside, peer, peer_beside, far, far_beside):
                arrived(step, b)
            staged[step, 2] = product(step, beside)
            for p in range(2):
                to_side_out(staged.at[step, 2, tile(p)], step, p).start()
            out[:, columns(x, step)] = product(step, band)

        def body(step, carry):
            @pl.when(step + 6 < steps)
            def _():
                mine(step + 6)
                side(step + 6)

            for p in range(2):
                to_pass(step, p).wait_recv()
                to_side_out(passing.at[step, tile(p)], step, p).start()
            return carry

        lax.fori_loop(ahead, steps, body, 0)

    def spread(hop):
        target = lax.rem(band + hop, nb)
        return send(part, parts.at[band], part_out.at[hop], part_in.at[band], at(target))

    for hop in range(1, nb):
        spread(hop).start()
    parts[band] = part[...]
    for hop in range(1, nb):
        source = lax.rem(band + nb - hop, nb)
        send(parts.at[source], parts.at[source], part_out.at[hop], part_in.at[source], at(source)).wait_recv()
    for of in range(2):
        total = parts[of]
        for level in range(1, nz):
            total = total + parts[2 * level + of]
        density[of] = total / jnp.float32(total_bands)

    def finish(step, carry):
        across(step).wait_send()
        for p in range(2):
            to_side_out(passing.at[step, tile(p)], step, p).wait_send()
            from_side_out(step, p)

        @pl.when(inner)
        def _():
            for i, b in enumerate((band, beside, mate, mate_beside)):
                block(step, b, peer_out.at[step, i], peer).wait_send()

            @pl.when(step < ahead)
            def _():
                for i, b in enumerate((band, beside, peer, peer_beside, far, far_beside)):
                    block(step, b, share_out.at[step, i], mate).wait_send()

            @pl.when(step >= ahead)
            def _():
                for p in range(2):
                    to_pass(step, p).wait_send()
                    to_mate_out(step, p).wait_send()

        @pl.when(outer)
        def _():
            for i, b in enumerate((band, beside)):
                block(step, b, mate_out.at[step, i], mate).wait_send()

            @pl.when(step >= ahead)
            def _():
                for p in range(2):
                    there = out.at[tile(p), columns(x, step)]
                    send(there, there, res_mate.at[step, p], mate_in.at[step, p], at(mate)).wait_recv()

        return carry

    lax.fori_loop(0, steps, finish, 0)
    for q in range(nz):
        to_core(0, band, q).wait_send()
        to_core(1, beside, q).wait_send()
        to_side(0, band, q).wait_send()

        @pl.when(inner)
        def _():
            to_core(2, mate, q).wait_send()
            to_core(3, mate_beside, q).wait_send()
            to_side(1, mate, q).wait_send()

        @pl.when(outer)
        def _():
            to_mate(q).wait_send()

    for hop in range(1, nb):
        spread(hop).wait_send()


def local(nb, wavefunctions, eigvec, occupation):
    rows, points = wavefunctions.shape
    total_bands, width = eigvec.shape
    steps = points // 2 // LANES
    if nb != 8 or width != LANES or rows != 2 * width or points % (2 * LANES) or steps < SHARED + 8 or total_bands != nb * rows:
        return plain(wavefunctions, eigvec, occupation)
    nz, deep = nb // 2, total_bands // (nb // 2)
    vmem = pl.BlockSpec(memory_space=pltpu.VMEM)
    hbm = pl.BlockSpec(memory_space=pltpu.HBM)
    dma = pltpu.SemaphoreType.DMA
    rotated, density = pl.pallas_call(
        kernel,
        out_shape=(
            pltpu.VMEM((rows, points), jnp.float32),
            pltpu.VMEM((2, steps, 1, LANES), jnp.float32),
        ),
        in_specs=[hbm] * 3,
        out_specs=(vmem, vmem),
        scratch_shapes=[
            pltpu.VMEM((steps, nb, rows, LANES), jnp.bfloat16),
            pltpu.VMEM((steps, rows, LANES), jnp.bfloat16),
            pltpu.VMEM((total_bands, width), jnp.bfloat16),
            pltpu.VMEM((nz, 4 * rows, deep), jnp.bfloat16),
            pltpu.VMEM((total_bands // LANES, LANES), jnp.float32),
            pltpu.VMEM((4 * rows, LANES), jnp.float32),
            pltpu.VMEM((steps, 3, rows, LANES), jnp.float32),
            pltpu.VMEM((steps, rows, LANES), jnp.float32),
            pltpu.VMEM((steps, 1, LANES), jnp.float32),
            pltpu.VMEM((nb, steps, 1, LANES), jnp.float32),
            dma((steps,)),
            dma((steps,)),
            dma((nz,)),
            dma((1,)),
            dma((steps, nb)),
            dma((steps,)),
            dma((steps, 4)),
            dma((steps, 2)),
            dma((SHARED, 6)),
            dma((8, nz)),
            dma((4, nz)),
            dma((2, nz)),
            dma((nz,)),
            dma((steps, 4)),
            dma((steps, 2)),
            dma((steps, 2)),
            dma((steps, 2)),
            dma((steps, 2)),
            dma((nb,)),
            dma((nb,)),
        ],
        compiler_params=pltpu.CompilerParams(
            collective_id=0, has_side_effects=True, vmem_limit_bytes=56 * 2**20
        ),
    )(wavefunctions, eigvec, occupation.reshape(total_bands // LANES, LANES))
    return (rotated, density.reshape(points))


def solution(mesh):
    placed = (P("band", ("frag", "slab")), P(None, ("frag", "band", "slab")), P("frag"))
    return jax.shard_map(
        functools.partial(local, mesh.shape["band"]),
        mesh=mesh,
        in_specs=placed,
        out_specs=(P("band", ("frag", "slab")), P(("frag", "slab"))),
        check_vma=False,
    )
```

```python
import functools

import jax
import jax.numpy as jnp
from jax import lax
from jax.experimental import pallas as pl
from jax.experimental.pallas import tpu as pltpu
from jax.sharding import PartitionSpec as P

MESH = pl.DeviceIdType.MESH
LANES = 128
SHARED = 3


def plain(wavefunctions, eigvec, occupation):
    total_bands = eigvec.shape[0]
    by_points = lax.all_to_all(wavefunctions, "band", split_axis=1, concat_axis=0, tiled=True)
    point_rows = lax.dot_general(
        lax.all_gather(eigvec, ("band", "slab"), axis=1, tiled=True),
        by_points,
        (((0,), (0,)), ((), ())),
        preferred_element_type=jnp.float32,
    )
    rotated = lax.all_to_all(point_rows, "band", split_axis=0, concat_axis=1, tiled=True)
    local_density = jnp.dot(
        occupation,
        point_rows * point_rows,
        precision=lax.Precision.HIGHEST,
        preferred_element_type=jnp.float32,
    ) / jnp.float32(total_bands)
    density = lax.all_gather(local_density, "band", axis=0, tiled=True)
    return (rotated, density)


def kernel(
    wave, eigvec, occupation, out, density,
    gathered, away, raw, vectors, seats, weight, staged, passing, part, parts,
    own_in, away_in, raw_in, seats_in, early, late, away_out, peer_out, mate_out, share_out,
    vec_in, vec_core_in, vec_core, vec_side, vec_mate, res_mate, pass_in, mate_in, side_in, side_out, kept, part_out, part_in,
):
    nb, nz = gathered.shape[1], gathered.shape[1] // 2
    frag, band, slab = (lax.axis_index(name) for name in ("frag", "band", "slab"))
    z, x = band // 2, lax.rem(band, 2)
    end = z // 2
    inner = (z == 1) | (z == 2)
    outer = (z == 0) | (z == 3)
    rows, points = wave.shape
    half = points // 2
    steps = half // LANES
    total_bands, width = eigvec.shape
    deep = total_bands // nz
    tall = rows // 2
    ahead = SHARED

    mate_z = 4 * end + 1 - z
    beside = band + 1 - 2 * x
    mate, mate_beside = 2 * mate_z + x, 2 * mate_z + 1 - x
    peer, peer_beside = 2 * (3 - z) + x, 2 * (3 - z) + 1 - x
    far, far_beside = 2 * (3 - mate_z) + x, 2 * (3 - mate_z) + 1 - x

    def at(b, s=slab):
        return (frag, b, s)

    def send(src, dst, ssem, rsem, target):
        return pltpu.make_async_remote_copy(
            src_ref=src, dst_ref=dst, send_sem=ssem, recv_sem=rsem, device_id=target, device_id_type=MESH
        )

    def columns(of, step):
        return pl.ds(pl.multiple_of(of * half + step * LANES, LANES), LANES)

    def settle(ref, sem):
        pltpu.make_async_copy(ref, ref, sem).wait()

    def own_load(step, i):
        return pltpu.make_async_copy(wave.at[:, columns(x, step)], gathered.at[step, band], own_in.at[i])

    def away_load(step, i):
        return pltpu.make_async_copy(wave.at[:, columns(1 - x, step)], away.at[step], away_in.at[i])

    raw_load = pltpu.make_async_copy(eigvec, raw, raw_in.at[0])
    seats_load = pltpu.make_async_copy(occupation, seats, seats_in.at[0])

    def block(step, b, sem, target, way):
        there = gathered.at[step, b]
        rsem = early.at[step, b] if isinstance(step, int) and step < ahead else late.at[step - ahead, way]
        return send(there, there, sem.at[0], rsem, at(target))

    def across(step):
        rsem = early.at[step, band] if isinstance(step, int) and step < ahead else late.at[step - ahead, 0]
        return send(away.at[step], gathered.at[step, band], away_out.at[0], rsem, at(beside))

    def arrived(step, bands, way):
        if isinstance(step, int) and step < ahead:
            for b in bands:
                settle(gathered.at[step, b], early.at[step, b])
        else:
            settle(gathered.at[step, pl.ds(0, len(bands))], late.at[step - ahead, way])

    def seat_of(b):
        return b - 4 * end

    def panel_at(b, s):
        return pl.ds(pl.multiple_of((seat_of(b) * 2 + s) * width, width), width)

    def to_core(b, q):
        there = vectors.at[q, panel_at(b, slab)]
        return send(there, there, vec_core.at[0], vec_core_in.at[seat_of(b)], at(band, 1 - slab))

    def panel(b, q, sem, target):
        there = vectors.at[q, panel_at(b, slab)]
        return send(there, there, sem.at[0], vec_in.at[seat_of(b), q], at(target))

    def panel_wait(b, q):
        settle(vectors.at[q, panel_at(b, slab)], vec_in.at[seat_of(b), q])

    def core_wait(b):
        settle(vectors.at[:, panel_at(b, 1 - slab)], vec_core_in.at[seat_of(b)])

    def tile(p):
        return pl.ds(p * tall, tall)

    def pass_sem(step, p):
        return pass_in.at[step - ahead + p * (step == steps - 1)]

    def to_pass(step, p):
        return send(staged.at[step, 0, tile(p)], passing.at[step, tile(p)], res_mate.at[0], pass_sem(step, p), at(mate))

    def to_mate_out(step, p):
        there = out.at[tile(p), columns(x, step)]
        return send(staged.at[step, 1, tile(p)], there, res_mate.at[0], mate_in.at[0], at(mate))

    def to_side_out(src, step, p):
        return send(src, out.at[tile(p), columns(x, step)], side_out.at[0], side_in.at[0], at(beside))

    def keep(step):
        return pltpu.make_async_copy(staged.at[step, 3], out.at[:, columns(x, step)], kept.at[0])

    def product(step, b):
        first = pl.multiple_of(seat_of(b) * rows, rows)
        total = None
        for q in range(nz):
            term = jnp.dot(
                vectors[q, pl.ds(first, rows), :],
                gathered[step, pl.ds(2 * q, 2)].reshape(deep, LANES),
                preferred_element_type=jnp.float32,
            )
            total = term if total is None else total + term
        part[step] = part[step] + jnp.sum(weight[pl.ds(first, rows), :] * total * total, axis=0, keepdims=True)
        return total

    def load(step, carry):
        i = step if isinstance(step, int) else ahead + 1
        away_load(step, i).start()
        own_load(step, i).start()
        return carry

    for step in range(ahead + 1):
        load(step, None)
    raw_load.start()
    seats_load.start()

    barrier = pltpu.get_barrier_semaphore()
    for target in (at(beside), at(mate), at(band, 1 - slab)):
        pl.semaphore_signal(barrier, inc=1, device_id=target, device_id_type=MESH)

    @pl.when(inner)
    def _():
        pl.semaphore_signal(barrier, inc=1, device_id=at(peer), device_id_type=MESH)
        pl.semaphore_wait(barrier, 4)

    @pl.when(outer)
    def _():
        pl.semaphore_wait(barrier, 3)

    def exchange(step):
        if isinstance(step, int) and step <= ahead:
            away_load(step, step).wait()
        across(step).start()

    def own_ready(step):
        if isinstance(step, int) and step <= ahead:
            own_load(step, step).wait()

    def rest_ready():
        others = pl.ds(ahead + 1, steps - ahead - 1)
        settle(away.at[others], away_in.at[ahead + 1])
        settle(away.at[others], own_in.at[ahead + 1])

    def turn():
        raw_load.wait()
        for q in range(nz):
            vectors[q, panel_at(band, slab), :] = raw[pl.ds(q * deep, deep), :].T

    def weigh():
        seats_load.wait()
        for group in range(8):
            row = seats[pl.ds(pl.multiple_of(8 * end, 8), 8), :][group : group + 1, :]
            weight[pl.ds(group * LANES, LANES), :] = jnp.broadcast_to(row, (LANES, LANES)).T

    part[...] = jnp.zeros(part.shape, part.dtype)

    def spread(hop):
        target = lax.rem(band + hop, nb)
        return send(part, parts.at[band], part_out.at[0], part_in.at[0], at(target))

    @pl.when(inner)
    def _():
        def onward(step, b):
            block(step, b, peer_out, peer, 2).start()

        def share(step, b):
            if isinstance(step, int) and step < ahead:
                block(step, b, share_out, mate, 1).start()

        def mine(step):
            own_ready(step)
            onward(step, band)
            share(step, band)

        def side(step):
            arrived(step, (beside,), 0)
            onward(step, beside)
            share(step, beside)

        def mates(step, which=(0, 1)):
            bands = [(mate, mate_beside)[i] for i in which]
            arrived(step, bands, 1)
            for b in bands:
                onward(step, b)

        def fars(step, which=(0, 1, 2, 3)):
            bands = [(peer, peer_beside, far, far_beside)[i] for i in which]
            arrived(step, bands, 2)
            for b in bands:
                share(step, b)

        def mate_panel(q):
            panel_wait(mate, q)
            panel(mate, q, vec_side, beside).start()
            to_core(mate, q).start()

        for step in range(ahead):
            mine(step)
            exchange(step)
        exchange(ahead)
        lax.fori_loop(ahead + 1, steps, load, 0)
        turn()
        for q in range(nz):
            to_core(band, q).start()
        rest_ready()
        exchange(4)
        exchange(5)
        for q in range(2):
            panel(band, q, vec_side, beside).start()
        weigh()
        for step in range(ahead):
            side(step)
            mates(step, (0,))
            fars(step, (0,))
        mine(3)
        for step in range(ahead):
            mates(step, (1,))
            fars(step, (1,))
        side(3)
        mates(3)
        mine(4)
        side(4)
        fars(0, (2, 3))
        mate_panel(0)
        fars(1, (2, 3))
        mate_panel(1)
        mine(5)
        side(5)
        fars(2, (2, 3))
        mate_panel(2)
        mate_panel(3)
        exchange(6)
        panel(band, 2, vec_side, beside).start()
        exchange(7)
        panel(band, 3, vec_side, beside).start()

        def for_mate(step):
            first = (step == ahead).astype(jnp.int32)
            for turn_of in range(2):
                slot = first * (1 - turn_of) + (1 - first) * turn_of
                b = 2 * mate_z + slot * x + (1 - slot) * (1 - x)

                @pl.when(step == ahead)
                def _():
                    if turn_of == 1:
                        mates(step + 1)
                        for q in range(nz):
                            panel_wait(mate_beside, q)
                            to_core(mate_beside, q).start()
                    core_wait((mate, mate_beside)[turn_of])

                staged[step, slot] = product(step, b)

                @pl.when(slot == 0)
                def _():
                    for p in range(2):
                        to_pass(step, p).start()

                @pl.when(slot == 1)
                def _():
                    for p in range(2):
                        to_mate_out(step, p).start()

        def for_row(step, carry):
            staged[step, 2] = product(step, beside)
            for p in range(2):
                to_side_out(staged.at[step, 2, tile(p)], step, p).start()
            staged[step, 3] = product(step, band)
            keep(step).start()
            return carry

        lag = ahead + 1

        def rows_done(step):
            return jnp.maximum(step + 1 - lag, 0) + jnp.minimum(jnp.maximum(step - 8, 0), lag)

        def body(step, carry):
            fars(step)
            for_mate(step)

            @pl.when((step > ahead) & (step + 1 < steps))
            def _():
                mates(step + 1)

            @pl.when((step >= 4) & (step + 2 < steps))
            def _():
                mine(step + 2)
                side(step + 2)

            @pl.when(step + 5 < steps)
            def _():
                exchange(step + 5)

            @pl.when(step == lag)
            def _():
                for q in range(nz):
                    panel_wait(beside, q)
                    to_core(beside, q).start()
                core_wait(band)
                core_wait(beside)

            lax.fori_loop(rows_done(step - 1), rows_done(step), for_row, 0)
            return carry

        lax.fori_loop(ahead, steps, body, 0)
        for hop in range(1, nb):
            spread(hop).start()

    @pl.when(outer)
    def _():
        def mine(step):
            own_ready(step)
            block(step, band, mate_out, mate, 1).start()

        def side(step):
            arrived(step, (beside,), 0)
            block(step, beside, mate_out, mate, 1).start()

        for step in range(ahead + 1):
            exchange(step)
            mine(step)
        lax.fori_loop(ahead + 1, steps, load, 0)
        turn()
        rest_ready()
        for step in range(ahead + 1, ahead + 5):
            exchange(step)
        for step in range(ahead + 1):
            side(step)
        for q in range(nz):
            panel(band, q, vec_mate, mate).start()
        for q in range(nz):
            panel(band, q, vec_side, beside).start()
            to_core(band, q).start()

        def begin(step, carry):
            exchange(step)
            return carry

        lax.fori_loop(ahead + 5, steps, begin, 0)
        weigh()
        for step in range(ahead + 1, ahead + 5):
            mine(step)
            side(step)
        for q in range(nz):
            panel_wait(beside, q)
            to_core(beside, q).start()
        core_wait(band)
        core_wait(beside)

        def shared(step, carry):
            for b in (mate, mate_beside, peer, peer_beside, far, far_beside):
                settle(gathered.at[step, b], early.at[step, b])
            staged[step, 2] = product(step, beside)
            for p in range(2):
                to_side_out(staged.at[step, 2, tile(p)], step, p).start()
            staged[step, 3] = product(step, band)
            keep(step).start()
            return carry

        lax.fori_loop(0, ahead, shared, 0)
        for hop in range(1, nb):
            spread(hop).start()

        def body(step, carry):
            @pl.when(step + 5 < steps)
            def _():
                mine(step + 5)
                side(step + 5)

            settle(passing.at[step], pass_in.at[step - ahead])
            for p in range(2):
                to_side_out(passing.at[step, tile(p)], step, p).start()
            return carry

        lax.fori_loop(ahead, steps - 1, body, 0)
        for p in range(2):
            settle(passing.at[steps - 1, tile(p)], pass_in.at[steps - 1 - ahead + p])
            to_side_out(passing.at[steps - 1, tile(p)], steps - 1, p).start()

    parts[band] = part[...]
    others = parts.at[pl.ds(0, nb - 1)]
    settle(others, part_in.at[0])
    for of in range(2):
        total = parts[of]
        for level in range(1, nz):
            total = total + parts[2 * level + of]
        density[of] = total / jnp.float32(total_bands)

    def blocks(n):
        return staged.at[pl.ds(0, n // 2), 0]

    settle(away, away_out.at[0])
    settle(others, part_out.at[0])

    @pl.when(inner)
    def _():
        settle(gathered.at[pl.ds(0, steps // 2)], peer_out.at[0])
        settle(blocks(6 * ahead), share_out.at[0])
        settle(vectors.at[:, pl.ds(0, 4 * width)], vec_core.at[0])
        settle(vectors.at[:, pl.ds(0, 2 * width)], vec_side.at[0])
        settle(staged.at[pl.ds(ahead, steps - ahead), pl.ds(0, 2)], res_mate.at[0])
        settle(blocks(2 * steps), kept.at[0])

    @pl.when(outer)
    def _():
        settle(blocks(2 * steps), mate_out.at[0])
        settle(vectors.at[:, pl.ds(0, 2 * width)], vec_core.at[0])
        settle(vectors.at[:, pl.ds(0, width)], vec_side.at[0])
        settle(vectors.at[:, pl.ds(0, width)], vec_mate.at[0])
        settle(blocks(2 * ahead), kept.at[0])
        settle(blocks(2 * (steps - ahead)), mate_in.at[0])

    settle(blocks(2 * steps), side_out.at[0])
    settle(blocks(2 * steps), side_in.at[0])


def local(nb, wavefunctions, eigvec, occupation):
    rows, points = wavefunctions.shape
    total_bands, width = eigvec.shape
    steps = points // 2 // LANES
    if nb != 8 or width != LANES or rows != 2 * width or points % (2 * LANES) or steps < SHARED + 8 or total_bands != nb * rows:
        return plain(wavefunctions, eigvec, occupation)
    nz, deep = nb // 2, total_bands // (nb // 2)
    vmem = pl.BlockSpec(memory_space=pltpu.VMEM)
    hbm = pl.BlockSpec(memory_space=pltpu.HBM)
    dma = pltpu.SemaphoreType.DMA
    rotated, density = pl.pallas_call(
        kernel,
        out_shape=(
            pltpu.VMEM((rows, points), jnp.float32),
            pltpu.VMEM((2, steps, 1, LANES), jnp.float32),
        ),
        in_specs=[hbm] * 3,
        out_specs=(pl.BlockSpec(memory_space=pl.ANY), vmem),
        scratch_shapes=[
            pltpu.VMEM((steps, nb, rows, LANES), jnp.bfloat16),
            pltpu.VMEM((steps, rows, LANES), jnp.bfloat16),
            pltpu.VMEM((total_bands, width), jnp.bfloat16),
            pltpu.VMEM((nz, 4 * rows, deep), jnp.bfloat16),
            pltpu.VMEM((total_bands // LANES, LANES), jnp.float32),
            pltpu.VMEM((4 * rows, LANES), jnp.float32),
            pltpu.VMEM((steps, 4, rows, LANES), jnp.float32),
            pltpu.VMEM((steps, rows, LANES), jnp.float32),
            pltpu.VMEM((steps, 1, LANES), jnp.float32),
            pltpu.VMEM((nb, steps, 1, LANES), jnp.float32),
            dma((SHARED + 2,)),
            dma((SHARED + 2,)),
            dma((1,)),
            dma((1,)),
            dma((SHARED, nb)),
            dma((steps - SHARED, 3)),
            *[dma((1,))] * 4,
            dma((4, nz)),
            dma((4,)),
            *[dma((1,))] * 4,
            dma((steps - SHARED + 1,)),
            *[dma((1,))] * 6,
        ],
        compiler_params=pltpu.CompilerParams(
            collective_id=0, has_side_effects=True, vmem_limit_bytes=56 * 2**20
        ),
    )(wavefunctions, eigvec, occupation.reshape(total_bands // LANES, LANES))
    return (rotated, density.reshape(points))


def solution(mesh):
    placed = (P("band", ("frag", "slab")), P(None, ("frag", "band", "slab")), P("frag"))
    return jax.shard_map(
        functools.partial(local, mesh.shape["band"]),
        mesh=mesh,
        in_specs=placed,
        out_specs=(P("band", ("frag", "slab")), P(("frag", "slab"))),
        check_vma=False,
    )
```

```python
import functools

import jax
import jax.numpy as jnp
from jax import lax
from jax.experimental import pallas as pl
from jax.experimental.pallas import tpu as pltpu
from jax.sharding import PartitionSpec as P

MESH = pl.DeviceIdType.MESH
LANES = 128
SHARED = 3


def plain(wavefunctions, eigvec, occupation):
    total_bands = eigvec.shape[0]
    by_points = lax.all_to_all(wavefunctions, "band", split_axis=1, concat_axis=0, tiled=True)
    point_rows = lax.dot_general(
        lax.all_gather(eigvec, ("band", "slab"), axis=1, tiled=True),
        by_points,
        (((0,), (0,)), ((), ())),
        preferred_element_type=jnp.float32,
    )
    rotated = lax.all_to_all(point_rows, "band", split_axis=0, concat_axis=1, tiled=True)
    local_density = jnp.dot(
        occupation,
        point_rows * point_rows,
        precision=lax.Precision.HIGHEST,
        preferred_element_type=jnp.float32,
    ) / jnp.float32(total_bands)
    density = lax.all_gather(local_density, "band", axis=0, tiled=True)
    return (rotated, density)


def kernel(
    wave, eigvec, occupation, out, density,
    gathered, away, raw, vectors, seats, weight, staged, passing, part, parts,
    own_in, away_in, raw_in, seats_in, early, late, away_out, peer_out, mate_out, share_out,
    vec_in, vec_core_in, vec_core, vec_side, vec_mate, res_mate, pass_in, mate_in, side_in, side_out, kept, part_out, part_in,
):
    nb, nz = gathered.shape[1], gathered.shape[1] // 2
    frag, band, slab = (lax.axis_index(name) for name in ("frag", "band", "slab"))
    z, x = band // 2, lax.rem(band, 2)
    end = z // 2
    inner = (z == 1) | (z == 2)
    outer = (z == 0) | (z == 3)
    rows, points = wave.shape
    half = points // 2
    steps = half // LANES
    total_bands, width = eigvec.shape
    deep = total_bands // nz
    tall = rows // 2
    ahead = SHARED

    mate_z = 4 * end + 1 - z
    beside = band + 1 - 2 * x
    mate, mate_beside = 2 * mate_z + x, 2 * mate_z + 1 - x
    peer, peer_beside = 2 * (3 - z) + x, 2 * (3 - z) + 1 - x
    far, far_beside = 2 * (3 - mate_z) + x, 2 * (3 - mate_z) + 1 - x

    def at(b, s=slab):
        return (frag, b, s)

    def send(src, dst, ssem, rsem, target):
        return pltpu.make_async_remote_copy(
            src_ref=src, dst_ref=dst, send_sem=ssem, recv_sem=rsem, device_id=target, device_id_type=MESH
        )

    def columns(of, step):
        return pl.ds(pl.multiple_of(of * half + step * LANES, LANES), LANES)

    def settle(ref, sem):
        pltpu.make_async_copy(ref, ref, sem).wait()

    def own_load(step, i):
        return pltpu.make_async_copy(wave.at[:, columns(x, step)], gathered.at[step, band], own_in.at[i])

    def away_load(step, i):
        return pltpu.make_async_copy(wave.at[:, columns(1 - x, step)], away.at[step], away_in.at[i])

    raw_load = pltpu.make_async_copy(eigvec, raw, raw_in.at[0])
    seats_load = pltpu.make_async_copy(occupation, seats, seats_in.at[0])

    def block(step, b, sem, target, way):
        there = gathered.at[step, b]
        rsem = early.at[step, b] if isinstance(step, int) and step < ahead else late.at[step - ahead, way]
        return send(there, there, sem.at[0], rsem, at(target))

    def across(step):
        rsem = early.at[step, band] if isinstance(step, int) and step < ahead else late.at[step - ahead, 0]
        return send(away.at[step], gathered.at[step, band], away_out.at[0], rsem, at(beside))

    def arrived(step, bands, way):
        if isinstance(step, int) and step < ahead:
            for b in bands:
                settle(gathered.at[step, b], early.at[step, b])
        else:
            settle(gathered.at[step, pl.ds(0, len(bands))], late.at[step - ahead, way])

    def seat_of(b):
        return b - 4 * end

    def panel_at(b, s):
        return pl.ds(pl.multiple_of((seat_of(b) * 2 + s) * width, width), width)

    def to_core(b, q):
        there = vectors.at[q, panel_at(b, slab)]
        return send(there, there, vec_core.at[0], vec_core_in.at[seat_of(b)], at(band, 1 - slab))

    def panel(b, q, sem, target):
        there = vectors.at[q, panel_at(b, slab)]
        return send(there, there, sem.at[0], vec_in.at[seat_of(b), q], at(target))

    def panel_wait(b, q):
        settle(vectors.at[q, panel_at(b, slab)], vec_in.at[seat_of(b), q])

    def core_wait(b):
        settle(vectors.at[:, panel_at(b, 1 - slab)], vec_core_in.at[seat_of(b)])

    def tile(p):
        return pl.ds(p * tall, tall)

    def pass_sem(step, p):
        return pass_in.at[step - ahead + p * (step == steps - 1)]

    def to_pass(step, p):
        return send(staged.at[step, 0, tile(p)], passing.at[step, tile(p)], res_mate.at[0], pass_sem(step, p), at(mate))

    def to_mate_out(step, p):
        there = out.at[tile(p), columns(x, step)]
        return send(staged.at[step, 1, tile(p)], there, res_mate.at[0], mate_in.at[0], at(mate))

    def to_side_out(src, step, p):
        return send(src, out.at[tile(p), columns(x, step)], side_out.at[0], side_in.at[0], at(beside))

    def keep(step):
        return pltpu.make_async_copy(staged.at[step, 3], out.at[:, columns(x, step)], kept.at[0])

    def product(step, b):
        first = pl.multiple_of(seat_of(b) * rows, rows)
        total = None
        for q in range(nz):
            term = jnp.dot(
                vectors[q, pl.ds(first, rows), :],
                gathered[step, pl.ds(2 * q, 2)].reshape(deep, LANES),
                preferred_element_type=jnp.float32,
            )
            total = term if total is None else total + term
        part[step] = part[step] + jnp.sum(weight[pl.ds(first, rows), :] * total * total, axis=0, keepdims=True)
        return total

    def load(step, carry):
        i = step if isinstance(step, int) else ahead + 1
        away_load(step, i).start()
        own_load(step, i).start()
        return carry

    for step in range(ahead + 1):
        load(step, None)
    raw_load.start()
    seats_load.start()

    barrier = pltpu.get_barrier_semaphore()
    for target in (at(beside), at(mate), at(band, 1 - slab)):
        pl.semaphore_signal(barrier, inc=1, device_id=target, device_id_type=MESH)

    @pl.when(inner)
    def _():
        pl.semaphore_signal(barrier, inc=1, device_id=at(peer), device_id_type=MESH)
        pl.semaphore_wait(barrier, 4)

    @pl.when(outer)
    def _():
        pl.semaphore_wait(barrier, 3)

    def exchange(step):
        if isinstance(step, int) and step <= ahead:
            away_load(step, step).wait()
        across(step).start()

    def own_ready(step):
        if isinstance(step, int) and step <= ahead:
            own_load(step, step).wait()

    def rest_ready():
        others = pl.ds(ahead + 1, steps - ahead - 1)
        settle(away.at[others], away_in.at[ahead + 1])
        settle(away.at[others], own_in.at[ahead + 1])

    def turn():
        raw_load.wait()
        for q in range(nz):
            vectors[q, panel_at(band, slab), :] = raw[pl.ds(q * deep, deep), :].T

    def weigh():
        seats_load.wait()
        for group in range(8):
            row = seats[pl.ds(pl.multiple_of(8 * end, 8), 8), :][group : group + 1, :]
            weight[pl.ds(group * LANES, LANES), :] = jnp.broadcast_to(row, (LANES, LANES)).T

    part[...] = jnp.zeros(part.shape, part.dtype)

    def spread(hop):
        target = lax.rem(band + hop, nb)
        return send(part, parts.at[band], part_out.at[0], part_in.at[0], at(target))

    @pl.when(inner)
    def _():
        def onward(step, b):
            block(step, b, peer_out, peer, 2).start()

        def share(step, b):
            if isinstance(step, int) and step < ahead:
                block(step, b, share_out, mate, 1).start()

        def mine(step):
            own_ready(step)
            onward(step, band)
            share(step, band)

        def side(step):
            arrived(step, (beside,), 0)
            onward(step, beside)
            share(step, beside)

        def mates(step, which=(0, 1)):
            bands = [(mate, mate_beside)[i] for i in which]
            arrived(step, bands, 1)
            for b in bands:
                onward(step, b)

        def fars(step, which=(0, 1, 2, 3)):
            bands = [(peer, peer_beside, far, far_beside)[i] for i in which]
            arrived(step, bands, 2)
            for b in bands:
                share(step, b)

        def mate_panel(q):
            panel_wait(mate, q)
            panel(mate, q, vec_side, beside).start()
            to_core(mate, q).start()

        for step in range(ahead):
            mine(step)
            exchange(step)
        exchange(ahead)
        lax.fori_loop(ahead + 1, steps, load, 0)
        turn()
        for q in range(nz):
            to_core(band, q).start()
        rest_ready()
        for step in range(4, 8):
            exchange(step)
        panel(band, 0, vec_side, beside).start()
        weigh()
        for step in range(ahead):
            side(step)
            mates(step, (0,))
            fars(step, (0,))
        mine(3)
        for step in range(ahead):
            mates(step, (1,))
            fars(step, (1,))
        side(3)
        mates(3)
        mine(4)
        side(4)
        fars(0, (2, 3))
        mate_panel(0)
        fars(1, (2, 3))
        mate_panel(1)
        mine(5)
        side(5)
        fars(2, (2, 3))
        mate_panel(2)
        mate_panel(3)

        def for_mate(step):
            first = (step == ahead).astype(jnp.int32)
            for turn_of in range(2):
                slot = first * (1 - turn_of) + (1 - first) * turn_of
                b = 2 * mate_z + slot * x + (1 - slot) * (1 - x)

                @pl.when(step == ahead)
                def _():
                    if turn_of == 1:
                        mates(step + 1)
                        mine(step + 3)
                        side(step + 3)
                        for q in range(nz):
                            panel_wait(mate_beside, q)
                            to_core(mate_beside, q).start()
                    core_wait((mate, mate_beside)[turn_of])
                    if turn_of == 1:
                        exchange(step + 5)
                        for q in range(1, nz):
                            panel(band, q, vec_side, beside).start()

                staged[step, slot] = product(step, b)

                @pl.when(slot == 0)
                def _():
                    for p in range(2):
                        to_pass(step, p).start()

                @pl.when(slot == 1)
                def _():
                    for p in range(2):
                        to_mate_out(step, p).start()

        def for_row(step, carry):
            staged[step, 2] = product(step, beside)
            for p in range(2):
                to_side_out(staged.at[step, 2, tile(p)], step, p).start()
            staged[step, 3] = product(step, band)
            keep(step).start()
            return carry

        lag = ahead + 2

        def rows_done(step):
            return jnp.maximum(step + 1 - lag, 0) + jnp.minimum(jnp.maximum(step - 4, 0) // 2, lag)

        def body(step, carry):
            fars(step)
            for_mate(step)

            @pl.when((step > ahead) & (step + 3 < steps))
            def _():
                mine(step + 3)
                side(step + 3)

            @pl.when(step + 2 < steps)
            def _():
                mates(step + 2)

            @pl.when((step > ahead) & (step + 5 < steps))
            def _():
                exchange(step + 5)

            @pl.when(step == lag)
            def _():
                for q in range(nz):
                    panel_wait(beside, q)
                    to_core(beside, q).start()
                core_wait(band)
                core_wait(beside)

            lax.fori_loop(rows_done(step - 1), rows_done(step), for_row, 0)
            return carry

        lax.fori_loop(ahead, steps, body, 0)
        for hop in range(1, nb):
            spread(hop).start()

    @pl.when(outer)
    def _():
        def mine(step):
            own_ready(step)
            block(step, band, mate_out, mate, 1).start()

        def side(step):
            arrived(step, (beside,), 0)
            block(step, beside, mate_out, mate, 1).start()

        for step in range(ahead + 1):
            exchange(step)
            mine(step)
        lax.fori_loop(ahead + 1, steps, load, 0)
        turn()
        rest_ready()
        for step in range(ahead + 1, ahead + 5):
            exchange(step)
        for step in range(ahead + 1):
            side(step)
        for q in range(nz):
            panel(band, q, vec_mate, mate).start()
        for q in range(nz):
            panel(band, q, vec_side, beside).start()
            to_core(band, q).start()

        def begin(step, carry):
            exchange(step)
            return carry

        lax.fori_loop(ahead + 5, steps, begin, 0)
        weigh()
        for step in range(ahead + 1, ahead + 5):
            mine(step)
            side(step)
        for q in range(nz):
            panel_wait(beside, q)
            to_core(beside, q).start()
        core_wait(band)
        core_wait(beside)

        def shared(step, carry):
            for b in (mate, mate_beside, peer, peer_beside, far, far_beside):
                settle(gathered.at[step, b], early.at[step, b])
            staged[step, 2] = product(step, beside)
            for p in range(2):
                to_side_out(staged.at[step, 2, tile(p)], step, p).start()
            staged[step, 3] = product(step, band)
            keep(step).start()
            return carry

        lax.fori_loop(0, ahead, shared, 0)
        for hop in range(1, nb):
            spread(hop).start()

        def body(step, carry):
            @pl.when(step + 5 < steps)
            def _():
                mine(step + 5)
                side(step + 5)

            settle(passing.at[step], pass_in.at[step - ahead])
            for p in range(2):
                to_side_out(passing.at[step, tile(p)], step, p).start()
            return carry

        lax.fori_loop(ahead, steps - 1, body, 0)
        for p in range(2):
            settle(passing.at[steps - 1, tile(p)], pass_in.at[steps - 1 - ahead + p])
            to_side_out(passing.at[steps - 1, tile(p)], steps - 1, p).start()

    parts[band] = part[...]
    others = parts.at[pl.ds(0, nb - 1)]
    settle(others, part_in.at[0])
    for of in range(2):
        total = parts[of]
        for level in range(1, nz):
            total = total + parts[2 * level + of]
        density[of] = total / jnp.float32(total_bands)

    def blocks(n):
        return staged.at[pl.ds(0, n // 2), 0]

    settle(away, away_out.at[0])
    settle(others, part_out.at[0])

    @pl.when(inner)
    def _():
        settle(gathered.at[pl.ds(0, steps // 2)], peer_out.at[0])
        settle(blocks(6 * ahead), share_out.at[0])
        settle(vectors.at[:, pl.ds(0, 4 * width)], vec_core.at[0])
        settle(vectors.at[:, pl.ds(0, 2 * width)], vec_side.at[0])
        settle(staged.at[pl.ds(ahead, steps - ahead), pl.ds(0, 2)], res_mate.at[0])
        settle(blocks(2 * steps), kept.at[0])

    @pl.when(outer)
    def _():
        settle(blocks(2 * steps), mate_out.at[0])
        settle(vectors.at[:, pl.ds(0, 2 * width)], vec_core.at[0])
        settle(vectors.at[:, pl.ds(0, width)], vec_side.at[0])
        settle(vectors.at[:, pl.ds(0, width)], vec_mate.at[0])
        settle(blocks(2 * ahead), kept.at[0])
        settle(blocks(2 * (steps - ahead)), mate_in.at[0])

    settle(blocks(2 * steps), side_out.at[0])
    settle(blocks(2 * steps), side_in.at[0])


def local(nb, wavefunctions, eigvec, occupation):
    rows, points = wavefunctions.shape
    total_bands, width = eigvec.shape
    steps = points // 2 // LANES
    if nb != 8 or width != LANES or rows != 2 * width or points % (2 * LANES) or steps < SHARED + 8 or total_bands != nb * rows:
        return plain(wavefunctions, eigvec, occupation)
    nz, deep = nb // 2, total_bands // (nb // 2)
    vmem = pl.BlockSpec(memory_space=pltpu.VMEM)
    hbm = pl.BlockSpec(memory_space=pltpu.HBM)
    dma = pltpu.SemaphoreType.DMA
    rotated, density = pl.pallas_call(
        kernel,
        out_shape=(
            pltpu.VMEM((rows, points), jnp.float32),
            pltpu.VMEM((2, steps, 1, LANES), jnp.float32),
        ),
        in_specs=[hbm] * 3,
        out_specs=(pl.BlockSpec(memory_space=pl.ANY), vmem),
        scratch_shapes=[
            pltpu.VMEM((steps, nb, rows, LANES), jnp.bfloat16),
            pltpu.VMEM((steps, rows, LANES), jnp.bfloat16),
            pltpu.VMEM((total_bands, width), jnp.bfloat16),
            pltpu.VMEM((nz, 4 * rows, deep), jnp.bfloat16),
            pltpu.VMEM((total_bands // LANES, LANES), jnp.float32),
            pltpu.VMEM((4 * rows, LANES), jnp.float32),
            pltpu.VMEM((steps, 4, rows, LANES), jnp.float32),
            pltpu.VMEM((steps, rows, LANES), jnp.float32),
            pltpu.VMEM((steps, 1, LANES), jnp.float32),
            pltpu.VMEM((nb, steps, 1, LANES), jnp.float32),
            dma((SHARED + 2,)),
            dma((SHARED + 2,)),
            dma((1,)),
            dma((1,)),
            dma((SHARED, nb)),
            dma((steps - SHARED, 3)),
            *[dma((1,))] * 4,
            dma((4, nz)),
            dma((4,)),
            *[dma((1,))] * 4,
            dma((steps - SHARED + 1,)),
            *[dma((1,))] * 6,
        ],
        compiler_params=pltpu.CompilerParams(
            collective_id=0, has_side_effects=True, vmem_limit_bytes=56 * 2**20
        ),
    )(wavefunctions, eigvec, occupation.reshape(total_bands // LANES, LANES))
    return (rotated, density.reshape(points))


def solution(mesh):
    placed = (P("band", ("frag", "slab")), P(None, ("frag", "band", "slab")), P("frag"))
    return jax.shard_map(
        functools.partial(local, mesh.shape["band"]),
        mesh=mesh,
        in_specs=placed,
        out_specs=(P("band", ("frag", "slab")), P(("frag", "slab"))),
        check_vma=False,
    )
```

```python
import functools

import jax
import jax.numpy as jnp
from jax import lax
from jax.experimental import pallas as pl
from jax.experimental.pallas import tpu as pltpu
from jax.sharding import PartitionSpec as P

MESH = pl.DeviceIdType.MESH
LANES = 128
PIECES = 8
SHARED = 3


def plain(wavefunctions, eigvec, occupation):
    total_bands = eigvec.shape[0]
    by_points = lax.all_to_all(wavefunctions, "band", split_axis=1, concat_axis=0, tiled=True)
    point_rows = lax.dot_general(
        lax.all_gather(eigvec, ("band", "slab"), axis=1, tiled=True),
        by_points,
        (((0,), (0,)), ((), ())),
        preferred_element_type=jnp.float32,
    )
    rotated = lax.all_to_all(point_rows, "band", split_axis=0, concat_axis=1, tiled=True)
    local_density = jnp.dot(
        occupation,
        point_rows * point_rows,
        precision=lax.Precision.HIGHEST,
        preferred_element_type=jnp.float32,
    ) / jnp.float32(total_bands)
    density = lax.all_gather(local_density, "band", axis=0, tiled=True)
    return (rotated, density)


def kernel(
    wave, eigvec, occupation, out, density,
    gathered, away, raw, vectors, seats, weight, staged, passing, part, parts,
    own_in, away_in, raw_in, seats_in, early, late, away_out, peer_out, mate_out, share_out,
    vec_in, vec_core_in, vec_core, vec_side, vec_mate, res_mate, pass_in, mate_in, side_in, side_out, kept, part_out, part_in,
):
    nb, nz = gathered.shape[1], gathered.shape[1] // 2
    frag, band, slab = (lax.axis_index(name) for name in ("frag", "band", "slab"))
    z, x = band // 2, lax.rem(band, 2)
    end = z // 2
    inner = (z == 1) | (z == 2)
    outer = (z == 0) | (z == 3)
    rows, points = wave.shape
    half = points // 2
    steps = half // LANES
    total_bands, width = eigvec.shape
    deep = total_bands // nz
    tall = rows // 2
    ahead = SHARED

    mate_z = 4 * end + 1 - z
    beside = band + 1 - 2 * x
    mate, mate_beside = 2 * mate_z + x, 2 * mate_z + 1 - x
    peer, peer_beside = 2 * (3 - z) + x, 2 * (3 - z) + 1 - x
    far, far_beside = 2 * (3 - mate_z) + x, 2 * (3 - mate_z) + 1 - x

    def at(b, s=slab):
        return (frag, b, s)

    def send(src, dst, ssem, rsem, target):
        return pltpu.make_async_remote_copy(
            src_ref=src, dst_ref=dst, send_sem=ssem, recv_sem=rsem, device_id=target, device_id_type=MESH
        )

    def columns(of, step):
        return pl.ds(pl.multiple_of(of * half + step * LANES, LANES), LANES)

    def settle(ref, sem):
        pltpu.make_async_copy(ref, ref, sem).wait()

    def own_load(step, i):
        return pltpu.make_async_copy(wave.at[:, columns(x, step)], gathered.at[step, band], own_in.at[i])

    def away_load(step, i):
        return pltpu.make_async_copy(wave.at[:, columns(1 - x, step)], away.at[step], away_in.at[i])

    raw_load = pltpu.make_async_copy(eigvec, raw, raw_in.at[0])
    seats_load = pltpu.make_async_copy(occupation, seats, seats_in.at[0])

    def block(step, b, sem, target, way):
        there = gathered.at[step, b]
        rsem = early.at[step, b] if isinstance(step, int) and step < ahead else late.at[step - ahead, way]
        return send(there, there, sem.at[0], rsem, at(target))

    def across(step):
        rsem = early.at[step, band] if isinstance(step, int) and step < ahead else late.at[step - ahead, 0]
        return send(away.at[step], gathered.at[step, band], away_out.at[0], rsem, at(beside))

    def arrived(step, bands, way):
        if isinstance(step, int) and step < ahead:
            for b in bands:
                settle(gathered.at[step, b], early.at[step, b])
        else:
            settle(gathered.at[step, pl.ds(0, len(bands))], late.at[step - ahead, way])

    def seat_of(b):
        return b - 4 * end

    def panel_at(b, s):
        return pl.ds(pl.multiple_of((seat_of(b) * 2 + s) * width, width), width)

    def to_core(b, q):
        there = vectors.at[q, panel_at(b, slab)]
        return send(there, there, vec_core.at[0], vec_core_in.at[seat_of(b)], at(band, 1 - slab))

    def panel(b, q, sem, target):
        there = vectors.at[q, panel_at(b, slab)]
        return send(there, there, sem.at[0], vec_in.at[seat_of(b), q], at(target))

    def panel_wait(b, q):
        settle(vectors.at[q, panel_at(b, slab)], vec_in.at[seat_of(b), q])

    def core_wait(b):
        settle(vectors.at[:, panel_at(b, 1 - slab)], vec_core_in.at[seat_of(b)])

    def tile(p):
        return pl.ds(p * tall, tall)

    def pass_sem(step, p):
        return pass_in.at[step - ahead + p * (step == steps - 1)]

    def to_pass(step, p):
        return send(staged.at[step, 0, tile(p)], passing.at[step, tile(p)], res_mate.at[0], pass_sem(step, p), at(mate))

    def to_mate_out(step, p):
        there = out.at[tile(p), columns(x, step)]
        return send(staged.at[step, 1, tile(p)], there, res_mate.at[0], mate_in.at[0], at(mate))

    def to_side_out(src, step, p):
        return send(src, out.at[tile(p), columns(x, step)], side_out.at[0], side_in.at[0], at(beside))

    def keep(step):
        return pltpu.make_async_copy(staged.at[step, 3], out.at[:, columns(x, step)], kept.at[0])

    def product(step, b):
        first = pl.multiple_of(seat_of(b) * rows, rows)
        total = None
        for q in range(nz):
            term = jnp.dot(
                vectors[q, pl.ds(first, rows), :],
                gathered[step, pl.ds(2 * q, 2)].reshape(deep, LANES),
                preferred_element_type=jnp.float32,
            )
            total = term if total is None else total + term
        part[step] = part[step] + jnp.sum(weight[pl.ds(first, rows), :] * total * total, axis=0, keepdims=True)
        return total

    def load(step, carry):
        i = step if isinstance(step, int) else ahead + 1
        away_load(step, i).start()
        own_load(step, i).start()
        return carry

    for step in range(ahead + 1):
        load(step, None)
    raw_load.start()
    seats_load.start()

    barrier = pltpu.get_barrier_semaphore()
    for target in (at(beside), at(mate), at(band, 1 - slab)):
        pl.semaphore_signal(barrier, inc=1, device_id=target, device_id_type=MESH)

    @pl.when(inner)
    def _():
        pl.semaphore_signal(barrier, inc=1, device_id=at(peer), device_id_type=MESH)
        pl.semaphore_wait(barrier, 4)

    @pl.when(outer)
    def _():
        pl.semaphore_wait(barrier, 3)

    def exchange(step):
        if isinstance(step, int) and step <= ahead:
            away_load(step, step).wait()
        across(step).start()

    def own_ready(step):
        if isinstance(step, int) and step <= ahead:
            own_load(step, step).wait()

    def rest_ready():
        others = pl.ds(ahead + 1, steps - ahead - 1)
        settle(away.at[others], away_in.at[ahead + 1])
        settle(away.at[others], own_in.at[ahead + 1])

    def turn():
        raw_load.wait()
        for q in range(nz):
            vectors[q, panel_at(band, slab), :] = raw[pl.ds(q * deep, deep), :].T

    def weigh():
        seats_load.wait()
        for group in range(8):
            row = seats[pl.ds(pl.multiple_of(8 * end, 8), 8), :][group : group + 1, :]
            weight[pl.ds(group * LANES, LANES), :] = jnp.broadcast_to(row, (LANES, LANES)).T

    part[...] = jnp.zeros(part.shape, part.dtype)

    def spread(hop):
        target = lax.rem(band + hop, nb)
        return send(part, parts.at[band], part_out.at[0], part_in.at[0], at(target))

    @pl.when(inner)
    def _():
        def onward(step, b):
            block(step, b, peer_out, peer, 2).start()

        def share(step, b):
            if isinstance(step, int) and step < ahead:
                block(step, b, share_out, mate, 1).start()

        def mine(step):
            own_ready(step)
            onward(step, band)
            share(step, band)

        def side(step):
            arrived(step, (beside,), 0)
            onward(step, beside)
            share(step, beside)

        def mates(step, which=(0, 1)):
            bands = [(mate, mate_beside)[i] for i in which]
            arrived(step, bands, 1)
            for b in bands:
                onward(step, b)

        def fars(step, which=(0, 1, 2, 3)):
            bands = [(peer, peer_beside, far, far_beside)[i] for i in which]
            arrived(step, bands, 2)
            for b in bands:
                share(step, b)

        def mate_panel(q):
            panel_wait(mate, q)
            panel(mate, q, vec_side, beside).start()
            to_core(mate, q).start()

        for step in range(ahead):
            mine(step)
            exchange(step)
        exchange(ahead)
        lax.fori_loop(ahead + 1, steps, load, 0)
        turn()
        for q in range(nz):
            to_core(band, q).start()
        rest_ready()
        for step in range(4, 8):
            exchange(step)
        panel(band, 0, vec_side, beside).start()
        weigh()
        for step in range(ahead):
            side(step)
            mates(step, (0,))
            fars(step, (0,))
        mine(3)
        for step in range(ahead):
            mates(step, (1,))
            fars(step, (1,))
        side(3)
        mates(3)
        mine(4)
        side(4)
        fars(0, (2, 3))
        mate_panel(0)
        fars(1, (2, 3))
        mate_panel(1)
        mine(5)
        side(5)
        fars(2, (2, 3))
        mate_panel(2)
        mate_panel(3)

        def for_mate(step):
            first = (step == ahead).astype(jnp.int32)
            for turn_of in range(2):
                slot = first * (1 - turn_of) + (1 - first) * turn_of
                b = 2 * mate_z + slot * x + (1 - slot) * (1 - x)

                @pl.when(step == ahead)
                def _():
                    if turn_of == 1:
                        mates(step + 1)
                        mine(step + 3)
                        side(step + 3)
                        for q in range(nz):
                            panel_wait(mate_beside, q)
                            to_core(mate_beside, q).start()
                    core_wait((mate, mate_beside)[turn_of])
                    if turn_of == 1:
                        exchange(step + 5)
                        for q in range(1, nz):
                            panel(band, q, vec_side, beside).start()

                staged[step, slot] = product(step, b)

                @pl.when(slot == 0)
                def _():
                    for p in range(2):
                        to_pass(step, p).start()

                @pl.when((slot == 1) & (step < steps - 2))
                def _():
                    for p in range(2):
                        to_mate_out(step, p).start()

        def for_row(step, carry):
            staged[step, 2] = product(step, beside)
            for p in range(2):
                to_side_out(staged.at[step, 2, tile(p)], step, p).start()
            staged[step, 3] = product(step, band)
            keep(step).start()
            return carry

        lag = ahead + 2

        def rows_done(step):
            return jnp.maximum(step + 1 - lag, 0) + jnp.minimum(jnp.maximum(step - 4, 0) // 2, lag)

        def body(step, carry):
            fars(step)
            for_mate(step)

            @pl.when((step > ahead) & (step + 3 < steps))
            def _():
                mine(step + 3)
                side(step + 3)

            @pl.when(step + 2 < steps)
            def _():
                mates(step + 2)

            @pl.when((step > ahead) & (step + 5 < steps))
            def _():
                exchange(step + 5)

            @pl.when(step == lag)
            def _():
                for q in range(nz):
                    panel_wait(beside, q)
                    to_core(beside, q).start()
                core_wait(band)
                core_wait(beside)

            lax.fori_loop(rows_done(step - 1), rows_done(step), for_row, 0)
            return carry

        lax.fori_loop(ahead, steps, body, 0)
        for hop in range(1, nb):
            spread(hop).start()
        for step in (steps - 2, steps - 1):
            for p in range(2):
                to_mate_out(step, p).start()

    @pl.when(outer)
    def _():
        def mine(step):
            own_ready(step)
            block(step, band, mate_out, mate, 1).start()

        def side(step):
            arrived(step, (beside,), 0)
            block(step, beside, mate_out, mate, 1).start()

        for step in range(ahead + 1):
            exchange(step)
            mine(step)
        lax.fori_loop(ahead + 1, steps, load, 0)
        turn()
        rest_ready()
        for step in range(ahead + 1, ahead + 5):
            exchange(step)
        for step in range(ahead + 1):
            side(step)
        for q in range(nz):
            panel(band, q, vec_mate, mate).start()
        for q in range(nz):
            panel(band, q, vec_side, beside).start()
            to_core(band, q).start()

        def begin(step, carry):
            exchange(step)
            return carry

        lax.fori_loop(ahead + 5, steps, begin, 0)
        weigh()
        for step in range(ahead + 1, ahead + 5):
            mine(step)
            side(step)
        for q in range(nz):
            panel_wait(beside, q)
            to_core(beside, q).start()
        core_wait(band)
        core_wait(beside)

        def shared(step, carry):
            for b in (mate, mate_beside, peer, peer_beside, far, far_beside):
                settle(gathered.at[step, b], early.at[step, b])
            staged[step, 2] = product(step, beside)
            for p in range(2):
                to_side_out(staged.at[step, 2, tile(p)], step, p).start()
            staged[step, 3] = product(step, band)
            keep(step).start()
            return carry

        lax.fori_loop(0, ahead, shared, 0)
        for hop in range(1, nb):
            spread(hop).start()

        def body(step, carry):
            @pl.when(step + 5 < steps)
            def _():
                mine(step + 5)
                side(step + 5)

            settle(passing.at[step], pass_in.at[step - ahead])
            for p in range(2):
                to_side_out(passing.at[step, tile(p)], step, p).start()
            return carry

        lax.fori_loop(ahead, steps - 1, body, 0)
        for p in range(2):
            settle(passing.at[steps - 1, tile(p)], pass_in.at[steps - 1 - ahead + p])
            to_side_out(passing.at[steps - 1, tile(p)], steps - 1, p).start()

    parts[band] = part[...]
    others = parts.at[pl.ds(0, nb - 1)]
    settle(others, part_in.at[0])
    for of in range(2):
        total = parts[of]
        for level in range(1, nz):
            total = total + parts[2 * level + of]
        density[of] = total / jnp.float32(total_bands)

    def blocks(n):
        return staged.at[pl.ds(0, n // 2), 0]

    settle(away, away_out.at[0])
    settle(others, part_out.at[0])

    @pl.when(inner)
    def _():
        settle(gathered.at[pl.ds(0, steps // 2)], peer_out.at[0])
        settle(blocks(6 * ahead), share_out.at[0])
        settle(vectors.at[:, pl.ds(0, 4 * width)], vec_core.at[0])
        settle(vectors.at[:, pl.ds(0, 2 * width)], vec_side.at[0])
        settle(staged.at[pl.ds(ahead, steps - ahead), pl.ds(0, 2)], res_mate.at[0])
        settle(blocks(2 * steps), kept.at[0])

    @pl.when(outer)
    def _():
        settle(blocks(2 * steps), mate_out.at[0])
        settle(vectors.at[:, pl.ds(0, 2 * width)], vec_core.at[0])
        settle(vectors.at[:, pl.ds(0, width)], vec_side.at[0])
        settle(vectors.at[:, pl.ds(0, width)], vec_mate.at[0])
        settle(blocks(2 * ahead), kept.at[0])
        settle(blocks(2 * (steps - ahead)), mate_in.at[0])

    settle(blocks(2 * steps), side_out.at[0])
    settle(blocks(2 * steps), side_in.at[0])


def flush(rotated, density, rotated_out, density_out, sems):
    band = rotated.shape[0] // PIECES
    copies = [
        pltpu.make_async_copy(rotated.at[pl.ds(i * band, band)], rotated_out.at[pl.ds(i * band, band)], sems.at[i])
        for i in range(PIECES)
    ]
    copies.append(pltpu.make_async_copy(density, density_out, sems.at[PIECES]))
    for copy in copies:
        copy.start()
    for copy in copies:
        copy.wait()


def local(nb, wavefunctions, eigvec, occupation):
    rows, points = wavefunctions.shape
    total_bands, width = eigvec.shape
    steps = points // 2 // LANES
    if nb != 8 or width != LANES or rows != 2 * width or points % (2 * LANES) or steps < SHARED + 8 or total_bands != nb * rows:
        return plain(wavefunctions, eigvec, occupation)
    nz, deep = nb // 2, total_bands // (nb // 2)
    vmem = pl.BlockSpec(memory_space=pltpu.VMEM)
    hbm = pl.BlockSpec(memory_space=pltpu.HBM)
    dma = pltpu.SemaphoreType.DMA
    rotated, density = pl.pallas_call(
        kernel,
        out_shape=(
            pltpu.VMEM((rows, points), jnp.float32),
            pltpu.VMEM((2, steps, 1, LANES), jnp.float32),
        ),
        in_specs=[hbm] * 3,
        out_specs=(pl.BlockSpec(memory_space=pl.ANY), vmem),
        scratch_shapes=[
            pltpu.VMEM((steps, nb, rows, LANES), jnp.bfloat16),
            pltpu.VMEM((steps, rows, LANES), jnp.bfloat16),
            pltpu.VMEM((total_bands, width), jnp.bfloat16),
            pltpu.VMEM((nz, 4 * rows, deep), jnp.bfloat16),
            pltpu.VMEM((total_bands // LANES, LANES), jnp.float32),
            pltpu.VMEM((4 * rows, LANES), jnp.float32),
            pltpu.VMEM((steps, 4, rows, LANES), jnp.float32),
            pltpu.VMEM((steps, rows, LANES), jnp.float32),
            pltpu.VMEM((steps, 1, LANES), jnp.float32),
            pltpu.VMEM((nb, steps, 1, LANES), jnp.float32),
            dma((SHARED + 2,)),
            dma((SHARED + 2,)),
            dma((1,)),
            dma((1,)),
            dma((SHARED, nb)),
            dma((steps - SHARED, 3)),
            *[dma((1,))] * 4,
            dma((4, nz)),
            dma((4,)),
            *[dma((1,))] * 4,
            dma((steps - SHARED + 1,)),
            *[dma((1,))] * 6,
        ],
        compiler_params=pltpu.CompilerParams(
            collective_id=0, has_side_effects=True, vmem_limit_bytes=56 * 2**20
        ),
    )(wavefunctions, eigvec, occupation.reshape(total_bands // LANES, LANES))
    rotated, density = pl.pallas_call(
        flush,
        out_shape=(
            jax.ShapeDtypeStruct(rotated.shape, rotated.dtype),
            jax.ShapeDtypeStruct(density.shape, density.dtype),
        ),
        in_specs=[pl.BlockSpec(memory_space=pl.ANY)] * 2,
        out_specs=(hbm, hbm),
        scratch_shapes=[dma((PIECES + 1,))],
        compiler_params=pltpu.CompilerParams(vmem_limit_bytes=2**20),
    )(rotated, density)
    return (rotated, density.reshape(points))


def solution(mesh):
    placed = (P("band", ("frag", "slab")), P(None, ("frag", "band", "slab")), P("frag"))
    return jax.shard_map(
        functools.partial(local, mesh.shape["band"]),
        mesh=mesh,
        in_specs=placed,
        out_specs=(P("band", ("frag", "slab")), P(("frag", "slab"))),
        check_vma=False,
    )
```

```python
import functools

import jax
import jax.numpy as jnp
from jax import lax
from jax.experimental import pallas as pl
from jax.experimental.pallas import tpu as pltpu
from jax.sharding import PartitionSpec as P

MESH = pl.DeviceIdType.MESH
LANES = 128
PIECES = 8
SHARED = 3


def plain(wavefunctions, eigvec, occupation):
    total_bands = eigvec.shape[0]
    by_points = lax.all_to_all(wavefunctions, "band", split_axis=1, concat_axis=0, tiled=True)
    point_rows = lax.dot_general(
        lax.all_gather(eigvec, ("band", "slab"), axis=1, tiled=True),
        by_points,
        (((0,), (0,)), ((), ())),
        preferred_element_type=jnp.float32,
    )
    rotated = lax.all_to_all(point_rows, "band", split_axis=0, concat_axis=1, tiled=True)
    local_density = jnp.dot(
        occupation,
        point_rows * point_rows,
        precision=lax.Precision.HIGHEST,
        preferred_element_type=jnp.float32,
    ) / jnp.float32(total_bands)
    density = lax.all_gather(local_density, "band", axis=0, tiled=True)
    return (rotated, density)


def kernel(
    wave, eigvec, occupation, out, density,
    gathered, away, raw, vectors, seats, weight, staged, passing, part, parts, halves,
    own_in, away_in, raw_in, seats_in, early, late, away_out, peer_out, mate_out, share_out,
    vec_in, vec_core_in, vec_core, vec_side, vec_mate, res_mate, pass_in, mate_in, side_in, side_out, kept, sum_out, sum_in,
):
    nb, nz = gathered.shape[1], gathered.shape[1] // 2
    frag, band, slab = (lax.axis_index(name) for name in ("frag", "band", "slab"))
    z, x = band // 2, lax.rem(band, 2)
    end = z // 2
    inner = (z == 1) | (z == 2)
    outer = (z == 0) | (z == 3)
    rows, points = wave.shape
    half = points // 2
    steps = half // LANES
    total_bands, width = eigvec.shape
    deep = total_bands // nz
    tall = rows // 2
    ahead = SHARED

    mate_z = 4 * end + 1 - z
    beside = band + 1 - 2 * x
    mate, mate_beside = 2 * mate_z + x, 2 * mate_z + 1 - x
    peer, peer_beside = 2 * (3 - z) + x, 2 * (3 - z) + 1 - x
    far, far_beside = 2 * (3 - mate_z) + x, 2 * (3 - mate_z) + 1 - x

    def at(b, s=slab):
        return (frag, b, s)

    def send(src, dst, ssem, rsem, target):
        return pltpu.make_async_remote_copy(
            src_ref=src, dst_ref=dst, send_sem=ssem, recv_sem=rsem, device_id=target, device_id_type=MESH
        )

    def columns(of, step):
        return pl.ds(pl.multiple_of(of * half + step * LANES, LANES), LANES)

    def settle(ref, sem):
        pltpu.make_async_copy(ref, ref, sem).wait()

    def own_load(step, i):
        return pltpu.make_async_copy(wave.at[:, columns(x, step)], gathered.at[step, band], own_in.at[i])

    def away_load(step, i):
        return pltpu.make_async_copy(wave.at[:, columns(1 - x, step)], away.at[step], away_in.at[i])

    raw_load = pltpu.make_async_copy(eigvec, raw, raw_in.at[0])
    seats_load = pltpu.make_async_copy(occupation, seats, seats_in.at[0])

    def block(step, b, sem, target, way):
        there = gathered.at[step, b]
        rsem = early.at[step, b] if isinstance(step, int) and step < ahead else late.at[step - ahead, way]
        return send(there, there, sem.at[0], rsem, at(target))

    def across(step):
        rsem = early.at[step, band] if isinstance(step, int) and step < ahead else late.at[step - ahead, 0]
        return send(away.at[step], gathered.at[step, band], away_out.at[0], rsem, at(beside))

    def arrived(step, bands, way):
        if isinstance(step, int) and step < ahead:
            for b in bands:
                settle(gathered.at[step, b], early.at[step, b])
        else:
            settle(gathered.at[step, pl.ds(0, len(bands))], late.at[step - ahead, way])

    def seat_of(b):
        return b - 4 * end

    def panel_at(b, s):
        return pl.ds(pl.multiple_of((seat_of(b) * 2 + s) * width, width), width)

    def to_core(b, q):
        there = vectors.at[q, panel_at(b, slab)]
        return send(there, there, vec_core.at[0], vec_core_in.at[seat_of(b)], at(band, 1 - slab))

    def panel(b, q, sem, target):
        there = vectors.at[q, panel_at(b, slab)]
        return send(there, there, sem.at[0], vec_in.at[seat_of(b), q], at(target))

    def panel_wait(b, q):
        settle(vectors.at[q, panel_at(b, slab)], vec_in.at[seat_of(b), q])

    def core_wait(b):
        settle(vectors.at[:, panel_at(b, 1 - slab)], vec_core_in.at[seat_of(b)])

    def tile(p):
        return pl.ds(p * tall, tall)

    def pass_sem(step, p):
        return pass_in.at[step - ahead + p * (step == steps - 1)]

    def to_pass(step, p):
        return send(staged.at[step, 0, tile(p)], passing.at[step, tile(p)], res_mate.at[0], pass_sem(step, p), at(mate))

    def to_mate_out(step, p):
        there = out.at[tile(p), columns(x, step)]
        return send(staged.at[step, 1, tile(p)], there, res_mate.at[0], mate_in.at[0], at(mate))

    def to_side_out(src, step, p):
        return send(src, out.at[tile(p), columns(x, step)], side_out.at[0], side_in.at[0], at(beside))

    def keep(step):
        return pltpu.make_async_copy(staged.at[step, 3], out.at[:, columns(x, step)], kept.at[0])

    def product(step, b):
        first = pl.multiple_of(seat_of(b) * rows, rows)
        total = None
        for q in range(nz):
            term = jnp.dot(
                vectors[q, pl.ds(first, rows), :],
                gathered[step, pl.ds(2 * q, 2)].reshape(deep, LANES),
                preferred_element_type=jnp.float32,
            )
            total = term if total is None else total + term
        part[step] = part[step] + jnp.sum(weight[pl.ds(first, rows), :] * total * total, axis=0, keepdims=True)
        return total

    def load(step, carry):
        i = step if isinstance(step, int) else ahead + 1
        away_load(step, i).start()
        own_load(step, i).start()
        return carry

    barrier = pltpu.get_barrier_semaphore()
    for target in (at(beside), at(mate), at(band, 1 - slab)):
        pl.semaphore_signal(barrier, inc=1, device_id=target, device_id_type=MESH)

    @pl.when(inner)
    def _():
        pl.semaphore_signal(barrier, inc=1, device_id=at(peer), device_id_type=MESH)

    for step in range(ahead + 1):
        load(step, None)
    raw_load.start()
    seats_load.start()

    @pl.when(inner)
    def _():
        pl.semaphore_wait(barrier, 4)

    @pl.when(outer)
    def _():
        pl.semaphore_wait(barrier, 3)

    def exchange(step):
        if isinstance(step, int) and step <= ahead:
            away_load(step, step).wait()
        across(step).start()

    def own_ready(step):
        if isinstance(step, int) and step <= ahead:
            own_load(step, step).wait()

    def rest_ready():
        others = pl.ds(ahead + 1, steps - ahead - 1)
        settle(away.at[others], away_in.at[ahead + 1])
        settle(away.at[others], own_in.at[ahead + 1])

    def turn():
        raw_load.wait()
        for q in range(nz):
            vectors[q, panel_at(band, slab), :] = raw[pl.ds(q * deep, deep), :].T

    def weigh():
        seats_load.wait()
        for group in range(8):
            row = seats[pl.ds(pl.multiple_of(8 * end, 8), 8), :][group : group + 1, :]
            weight[pl.ds(group * LANES, LANES), :] = jnp.broadcast_to(row, (LANES, LANES)).T

    part[...] = jnp.zeros(part.shape, part.dtype)

    first_steps = pl.ds(0, ahead)

    def sum_to_mate():
        return send(part.at[first_steps], parts.at[0, first_steps], sum_out.at[0], sum_in.at[0], at(mate))

    def sum_to_peer():
        return send(part, parts.at[1], sum_out.at[0], sum_in.at[1], at(peer))

    def total_to(b, i):
        return send(halves.at[x], halves.at[x], sum_out.at[1], sum_in.at[i], at(b))

    @pl.when(inner)
    def _():
        def onward(step, b):
            block(step, b, peer_out, peer, 2).start()

        def share(step, b):
            if isinstance(step, int) and step < ahead:
                block(step, b, share_out, mate, 1).start()

        def mine(step):
            own_ready(step)
            onward(step, band)
            share(step, band)

        def side(step):
            arrived(step, (beside,), 0)
            onward(step, beside)
            share(step, beside)

        def mates(step, which=(0, 1)):
            bands = [(mate, mate_beside)[i] for i in which]
            arrived(step, bands, 1)
            for b in bands:
                onward(step, b)

        def fars(step, which=(0, 1, 2, 3)):
            bands = [(peer, peer_beside, far, far_beside)[i] for i in which]
            arrived(step, bands, 2)
            for b in bands:
                share(step, b)

        def mate_panel(q):
            panel_wait(mate, q)
            panel(mate, q, vec_side, beside).start()
            to_core(mate, q).start()

        for step in range(ahead):
            mine(step)
            exchange(step)
        exchange(ahead)
        lax.fori_loop(ahead + 1, steps, load, 0)
        turn()
        for q in range(nz):
            to_core(band, q).start()
        rest_ready()
        for step in range(4, 8):
            exchange(step)
        panel(band, 0, vec_side, beside).start()
        weigh()
        for step in range(ahead):
            side(step)
            mates(step, (0,))
            fars(step, (0,))
        mine(3)
        for step in range(ahead):
            mates(step, (1,))
            fars(step, (1,))
        side(3)
        mates(3)
        mine(4)
        side(4)
        fars(0, (2, 3))
        mate_panel(0)
        fars(1, (2, 3))
        mate_panel(1)
        mine(5)
        side(5)
        fars(2, (2, 3))
        mate_panel(2)
        mate_panel(3)

        def for_mate(step):
            first = (step == ahead).astype(jnp.int32)
            for turn_of in range(2):
                slot = first * (1 - turn_of) + (1 - first) * turn_of
                b = 2 * mate_z + slot * x + (1 - slot) * (1 - x)

                @pl.when(step == ahead)
                def _():
                    if turn_of == 1:
                        mates(step + 1)
                        mine(step + 3)
                        side(step + 3)
                        for q in range(nz):
                            panel_wait(mate_beside, q)
                            to_core(mate_beside, q).start()
                    core_wait((mate, mate_beside)[turn_of])
                    if turn_of == 1:
                        exchange(step + 5)
                        for q in range(1, nz):
                            panel(band, q, vec_side, beside).start()

                staged[step, slot] = product(step, b)

                @pl.when(slot == 0)
                def _():
                    for p in range(2):
                        to_pass(step, p).start()

                    @pl.when(step == steps - 1)
                    def _():
                        for p in range(2):
                            to_mate_out(step - 1, p).start()

                @pl.when((slot == 1) & (step < steps - 2))
                def _():
                    for p in range(2):
                        to_mate_out(step, p).start()

        def for_row(step, carry):
            staged[step, 2] = product(step, beside)
            for p in range(2):
                to_side_out(staged.at[step, 2, tile(p)], step, p).start()
            staged[step, 3] = product(step, band)
            keep(step).start()
            return carry

        lag = ahead + 2

        def rows_done(step):
            return jnp.maximum(step + 1 - lag, 0) + jnp.minimum(jnp.maximum(step - 4, 0) // 2, lag)

        def body(step, carry):
            fars(step)
            for_mate(step)

            @pl.when((step > ahead) & (step + 3 < steps))
            def _():
                mine(step + 3)
                side(step + 3)

            @pl.when(step + 2 < steps)
            def _():
                mates(step + 2)

            @pl.when((step > ahead) & (step + 5 < steps))
            def _():
                exchange(step + 5)

            @pl.when(step == lag)
            def _():
                for q in range(nz):
                    panel_wait(beside, q)
                    to_core(beside, q).start()
                core_wait(band)
                core_wait(beside)

            lax.fori_loop(rows_done(step - 1), rows_done(step), for_row, 0)
            return carry

        lax.fori_loop(ahead, steps, body, 0)
        settle(parts.at[0, first_steps], sum_in.at[0])
        part[first_steps] = part[first_steps] + parts[0, first_steps]
        sum_to_peer().start()
        settle(parts.at[1], sum_in.at[1])
        halves[x] = (part[...] + parts[1]) / jnp.float32(total_bands)
        total_to(mate_beside, 3).start()
        total_to(mate, 2).start()
        total_to(beside, 3).start()
        for p in range(2):
            to_mate_out(steps - 1, p).start()

    @pl.when(outer)
    def _():
        def mine(step):
            own_ready(step)
            block(step, band, mate_out, mate, 1).start()

        def side(step):
            arrived(step, (beside,), 0)
            block(step, beside, mate_out, mate, 1).start()

        for step in range(ahead + 1):
            exchange(step)
            mine(step)
        lax.fori_loop(ahead + 1, steps, load, 0)
        turn()
        rest_ready()
        for step in range(ahead + 1, ahead + 5):
            exchange(step)
        for step in range(ahead + 1):
            side(step)
        for q in range(nz):
            panel(band, q, vec_mate, mate).start()
        for q in range(nz):
            panel(band, q, vec_side, beside).start()
            to_core(band, q).start()

        def begin(step, carry):
            exchange(step)
            return carry

        lax.fori_loop(ahead + 5, steps, begin, 0)
        weigh()
        for step in range(ahead + 1, ahead + 5):
            mine(step)
            side(step)
        for q in range(nz):
            panel_wait(beside, q)
            to_core(beside, q).start()
        core_wait(band)
        core_wait(beside)

        def shared(step, carry):
            for b in (mate, mate_beside, peer, peer_beside, far, far_beside):
                settle(gathered.at[step, b], early.at[step, b])
            staged[step, 2] = product(step, beside)
            for p in range(2):
                to_side_out(staged.at[step, 2, tile(p)], step, p).start()
            staged[step, 3] = product(step, band)
            keep(step).start()
            return carry

        lax.fori_loop(0, ahead, shared, 0)
        sum_to_mate().start()

        def body(step, carry):
            @pl.when(step + 5 < steps)
            def _():
                mine(step + 5)
                side(step + 5)

            settle(passing.at[step], pass_in.at[step - ahead])
            for p in range(2):
                to_side_out(passing.at[step, tile(p)], step, p).start()
            return carry

        lax.fori_loop(ahead, steps - 1, body, 0)
        for p in range(2):
            settle(passing.at[steps - 1, tile(p)], pass_in.at[steps - 1 - ahead + p])
            to_side_out(passing.at[steps - 1, tile(p)], steps - 1, p).start()

    @pl.when(outer)
    def _():
        settle(halves.at[x], sum_in.at[2])

    settle(halves.at[1 - x], sum_in.at[3])
    density[...] = halves[...]

    def blocks(n):
        return staged.at[pl.ds(0, n // 2), 0]

    settle(away, away_out.at[0])

    @pl.when(inner)
    def _():
        settle(gathered.at[pl.ds(0, steps // 2)], peer_out.at[0])
        settle(part, sum_out.at[0])
        settle(parts, sum_out.at[1])
        settle(blocks(6 * ahead), share_out.at[0])
        settle(vectors.at[:, pl.ds(0, 4 * width)], vec_core.at[0])
        settle(vectors.at[:, pl.ds(0, 2 * width)], vec_side.at[0])
        settle(staged.at[pl.ds(ahead, steps - ahead), pl.ds(0, 2)], res_mate.at[0])
        settle(blocks(2 * steps), kept.at[0])

    @pl.when(outer)
    def _():
        settle(part.at[first_steps], sum_out.at[0])
        settle(blocks(2 * steps), mate_out.at[0])
        settle(vectors.at[:, pl.ds(0, 2 * width)], vec_core.at[0])
        settle(vectors.at[:, pl.ds(0, width)], vec_side.at[0])
        settle(vectors.at[:, pl.ds(0, width)], vec_mate.at[0])
        settle(blocks(2 * ahead), kept.at[0])
        settle(blocks(2 * (steps - ahead)), mate_in.at[0])

    settle(blocks(2 * steps), side_out.at[0])
    settle(blocks(2 * steps), side_in.at[0])


def flush(rotated, density, rotated_out, density_out, sems):
    band = rotated.shape[0] // PIECES
    copies = [
        pltpu.make_async_copy(rotated.at[pl.ds(i * band, band)], rotated_out.at[pl.ds(i * band, band)], sems.at[i])
        for i in range(PIECES)
    ]
    copies.append(pltpu.make_async_copy(density, density_out, sems.at[PIECES]))
    for copy in copies:
        copy.start()
    for copy in copies:
        copy.wait()


def local(nb, wavefunctions, eigvec, occupation):
    rows, points = wavefunctions.shape
    total_bands, width = eigvec.shape
    steps = points // 2 // LANES
    if nb != 8 or width != LANES or rows != 2 * width or points % (2 * LANES) or steps < SHARED + 8 or total_bands != nb * rows:
        return plain(wavefunctions, eigvec, occupation)
    nz, deep = nb // 2, total_bands // (nb // 2)
    vmem = pl.BlockSpec(memory_space=pltpu.VMEM)
    hbm = pl.BlockSpec(memory_space=pltpu.HBM)
    dma = pltpu.SemaphoreType.DMA
    rotated, density = pl.pallas_call(
        kernel,
        out_shape=(
            pltpu.VMEM((rows, points), jnp.float32),
            pltpu.VMEM((2, steps, 1, LANES), jnp.float32),
        ),
        in_specs=[hbm] * 3,
        out_specs=(pl.BlockSpec(memory_space=pl.ANY), vmem),
        scratch_shapes=[
            pltpu.VMEM((steps, nb, rows, LANES), jnp.bfloat16),
            pltpu.VMEM((steps, rows, LANES), jnp.bfloat16),
            pltpu.VMEM((total_bands, width), jnp.bfloat16),
            pltpu.VMEM((nz, 4 * rows, deep), jnp.bfloat16),
            pltpu.VMEM((total_bands // LANES, LANES), jnp.float32),
            pltpu.VMEM((4 * rows, LANES), jnp.float32),
            pltpu.VMEM((steps, 4, rows, LANES), jnp.float32),
            pltpu.VMEM((steps, rows, LANES), jnp.float32),
            pltpu.VMEM((steps, 1, LANES), jnp.float32),
            pltpu.VMEM((3, steps, 1, LANES), jnp.float32),
            pltpu.VMEM((2, steps, 1, LANES), jnp.float32),
            dma((SHARED + 2,)),
            dma((SHARED + 2,)),
            dma((1,)),
            dma((1,)),
            dma((SHARED, nb)),
            dma((steps - SHARED, 3)),
            *[dma((1,))] * 4,
            dma((4, nz)),
            dma((4,)),
            *[dma((1,))] * 4,
            dma((steps - SHARED + 1,)),
            *[dma((1,))] * 4,
            dma((2,)),
            dma((4,)),
        ],
        compiler_params=pltpu.CompilerParams(
            collective_id=0, has_side_effects=True, vmem_limit_bytes=56 * 2**20
        ),
    )(wavefunctions, eigvec, occupation.reshape(total_bands // LANES, LANES))
    rotated, density = pl.pallas_call(
        flush,
        out_shape=(
            jax.ShapeDtypeStruct(rotated.shape, rotated.dtype),
            jax.ShapeDtypeStruct(density.shape, density.dtype),
        ),
        in_specs=[pl.BlockSpec(memory_space=pl.ANY)] * 2,
        out_specs=(hbm, hbm),
        scratch_shapes=[dma((PIECES + 1,))],
        compiler_params=pltpu.CompilerParams(vmem_limit_bytes=2**20),
    )(rotated, density)
    return (rotated, density.reshape(points))


def solution(mesh):
    placed = (P("band", ("frag", "slab")), P(None, ("frag", "band", "slab")), P("frag"))
    return jax.shard_map(
        functools.partial(local, mesh.shape["band"]),
        mesh=mesh,
        in_specs=placed,
        out_specs=(P("band", ("frag", "slab")), P(("frag", "slab"))),
        check_vma=False,
    )
```

```python
import functools

import jax
import jax.numpy as jnp
from jax import lax
from jax.experimental import pallas as pl
from jax.experimental.pallas import tpu as pltpu
from jax.sharding import PartitionSpec as P

MESH = pl.DeviceIdType.MESH
LANES = 128
PIECES = 8
SHARED = 3


def plain(wavefunctions, eigvec, occupation):
    total_bands = eigvec.shape[0]
    by_points = lax.all_to_all(wavefunctions, "band", split_axis=1, concat_axis=0, tiled=True)
    point_rows = lax.dot_general(
        lax.all_gather(eigvec, ("band", "slab"), axis=1, tiled=True),
        by_points,
        (((0,), (0,)), ((), ())),
        preferred_element_type=jnp.float32,
    )
    rotated = lax.all_to_all(point_rows, "band", split_axis=0, concat_axis=1, tiled=True)
    local_density = jnp.dot(
        occupation,
        point_rows * point_rows,
        precision=lax.Precision.HIGHEST,
        preferred_element_type=jnp.float32,
    ) / jnp.float32(total_bands)
    density = lax.all_gather(local_density, "band", axis=0, tiled=True)
    return (rotated, density)


def kernel(
    wave, eigvec, occupation, out, density,
    gathered, away, raw, vectors, seats, weight, staged, passing, part, parts, halves,
    own_in, away_in, raw_in, seats_in, early, late, away_out, peer_out, mate_out, share_out,
    vec_in, vec_core_in, vec_core, vec_side, vec_mate, res_mate, pass_in, mate_in, side_in, side_out, kept, sum_out, sum_in,
):
    nb, nz = gathered.shape[1], gathered.shape[1] // 2
    frag, band, slab = (lax.axis_index(name) for name in ("frag", "band", "slab"))
    z, x = band // 2, lax.rem(band, 2)
    end = z // 2
    inner = (z == 1) | (z == 2)
    outer = (z == 0) | (z == 3)
    rows, points = wave.shape
    half = points // 2
    steps = half // LANES
    total_bands, width = eigvec.shape
    deep = total_bands // nz
    tall = rows // 2
    ahead = SHARED

    mate_z = 4 * end + 1 - z
    beside = band + 1 - 2 * x
    mate, mate_beside = 2 * mate_z + x, 2 * mate_z + 1 - x
    peer, peer_beside = 2 * (3 - z) + x, 2 * (3 - z) + 1 - x
    far, far_beside = 2 * (3 - mate_z) + x, 2 * (3 - mate_z) + 1 - x

    def at(b, s=slab):
        return (frag, b, s)

    def send(src, dst, ssem, rsem, target):
        return pltpu.make_async_remote_copy(
            src_ref=src, dst_ref=dst, send_sem=ssem, recv_sem=rsem, device_id=target, device_id_type=MESH
        )

    def columns(of, step):
        return pl.ds(pl.multiple_of(of * half + step * LANES, LANES), LANES)

    def settle(ref, sem):
        pltpu.make_async_copy(ref, ref, sem).wait()

    def own_load(step, i):
        return pltpu.make_async_copy(wave.at[:, columns(x, step)], gathered.at[step, band], own_in.at[i])

    def away_load(step, i):
        return pltpu.make_async_copy(wave.at[:, columns(1 - x, step)], away.at[step], away_in.at[i])

    raw_load = pltpu.make_async_copy(eigvec, raw, raw_in.at[0])
    seats_load = pltpu.make_async_copy(occupation, seats, seats_in.at[0])

    def block(step, b, sem, target, way):
        there = gathered.at[step, b]
        rsem = early.at[step, b] if isinstance(step, int) and step < ahead else late.at[step - ahead, way]
        return send(there, there, sem.at[0], rsem, at(target))

    def across(step):
        rsem = early.at[step, band] if isinstance(step, int) and step < ahead else late.at[step - ahead, 0]
        return send(away.at[step], gathered.at[step, band], away_out.at[0], rsem, at(beside))

    def arrived(step, bands, way):
        if isinstance(step, int) and step < ahead:
            for b in bands:
                settle(gathered.at[step, b], early.at[step, b])
        else:
            settle(gathered.at[step, pl.ds(0, len(bands))], late.at[step - ahead, way])

    def seat_of(b):
        return b - 4 * end

    def panel_at(b, s):
        return pl.ds(pl.multiple_of((seat_of(b) * 2 + s) * width, width), width)

    def to_core(b, q):
        there = vectors.at[q, panel_at(b, slab)]
        return send(there, there, vec_core.at[0], vec_core_in.at[seat_of(b)], at(band, 1 - slab))

    def panel(b, q, sem, target):
        there = vectors.at[q, panel_at(b, slab)]
        return send(there, there, sem.at[0], vec_in.at[seat_of(b), q], at(target))

    def panel_wait(b, q):
        settle(vectors.at[q, panel_at(b, slab)], vec_in.at[seat_of(b), q])

    def core_wait(b):
        settle(vectors.at[:, panel_at(b, 1 - slab)], vec_core_in.at[seat_of(b)])

    def tile(p):
        return pl.ds(p * tall, tall)

    def pass_sem(step, p):
        return pass_in.at[step - ahead + p * (step == steps - 1)]

    def to_pass(step, p):
        return send(staged.at[step, 0, tile(p)], passing.at[step, tile(p)], res_mate.at[0], pass_sem(step, p), at(mate))

    def to_mate_out(step, p):
        there = out.at[tile(p), columns(x, step)]
        return send(staged.at[step, 1, tile(p)], there, res_mate.at[0], mate_in.at[0], at(mate))

    def to_side_out(src, step, p):
        return send(src, out.at[tile(p), columns(x, step)], side_out.at[0], side_in.at[0], at(beside))

    def keep(step):
        return pltpu.make_async_copy(staged.at[step, 3], out.at[:, columns(x, step)], kept.at[0])

    def product(step, b):
        first = pl.multiple_of(seat_of(b) * rows, rows)
        total = None
        for q in range(nz):
            term = jnp.dot(
                vectors[q, pl.ds(first, rows), :],
                gathered[step, pl.ds(2 * q, 2)].reshape(deep, LANES),
                preferred_element_type=jnp.float32,
            )
            total = term if total is None else total + term
        part[step] = part[step] + jnp.sum(weight[pl.ds(first, rows), :] * total * total, axis=0, keepdims=True)
        return total

    def load(step, carry):
        i = step if isinstance(step, int) else ahead + 1
        away_load(step, i).start()
        own_load(step, i).start()
        return carry

    barrier = pltpu.get_barrier_semaphore()
    for target in (at(beside), at(mate), at(band, 1 - slab)):
        pl.semaphore_signal(barrier, inc=1, device_id=target, device_id_type=MESH)

    @pl.when(inner)
    def _():
        pl.semaphore_signal(barrier, inc=1, device_id=at(peer), device_id_type=MESH)

    for step in range(ahead + 1):
        load(step, None)
    raw_load.start()
    seats_load.start()

    @pl.when(inner)
    def _():
        pl.semaphore_wait(barrier, 4)

    @pl.when(outer)
    def _():
        pl.semaphore_wait(barrier, 3)

    def exchange(step):
        if isinstance(step, int) and step <= ahead:
            away_load(step, step).wait()
        across(step).start()

    def own_ready(step):
        if isinstance(step, int) and step <= ahead:
            own_load(step, step).wait()

    def rest_ready():
        others = pl.ds(ahead + 1, steps - ahead - 1)
        settle(away.at[others], away_in.at[ahead + 1])
        settle(away.at[others], own_in.at[ahead + 1])

    def turn():
        raw_load.wait()
        for q in range(nz):
            vectors[q, panel_at(band, slab), :] = raw[pl.ds(q * deep, deep), :].T

    def weigh():
        seats_load.wait()
        for group in range(8):
            row = seats[pl.ds(pl.multiple_of(8 * end, 8), 8), :][group : group + 1, :]
            weight[pl.ds(group * LANES, LANES), :] = jnp.broadcast_to(row, (LANES, LANES)).T

    part[...] = jnp.zeros(part.shape, part.dtype)

    first_steps = pl.ds(0, ahead)

    def sum_to_mate():
        return send(part.at[first_steps], parts.at[0, first_steps], sum_out.at[0], sum_in.at[0], at(mate))

    def sum_to_peer():
        return send(part, parts.at[1], sum_out.at[0], sum_in.at[1], at(peer))

    def total_to(b, i):
        return send(halves.at[x], halves.at[x], sum_out.at[1], sum_in.at[i], at(b))

    @pl.when(inner)
    def _():
        def onward(step, b):
            block(step, b, peer_out, peer, 2).start()

        def share(step, b):
            if isinstance(step, int) and step < ahead:
                block(step, b, share_out, mate, 1).start()

        def mine(step):
            own_ready(step)
            onward(step, band)
            share(step, band)

        def side(step):
            arrived(step, (beside,), 0)
            onward(step, beside)
            share(step, beside)

        def mates(step, which=(0, 1)):
            bands = [(mate, mate_beside)[i] for i in which]
            arrived(step, bands, 1)
            for b in bands:
                onward(step, b)

        def fars(step, which=(0, 1, 2, 3)):
            bands = [(peer, peer_beside, far, far_beside)[i] for i in which]
            arrived(step, bands, 2)
            for b in bands:
                share(step, b)

        def mate_panel(q):
            panel_wait(mate, q)
            panel(mate, q, vec_side, beside).start()
            to_core(mate, q).start()

        for step in range(ahead):
            mine(step)
            exchange(step)
        exchange(ahead)
        lax.fori_loop(ahead + 1, steps, load, 0)
        turn()
        for q in range(nz):
            to_core(band, q).start()
        rest_ready()
        for step in range(4, 8):
            exchange(step)
        panel(band, 0, vec_side, beside).start()
        weigh()
        for step in range(ahead):
            side(step)
            mates(step, (0,))
            fars(step, (0,))
        mine(3)
        for step in range(ahead):
            mates(step, (1,))
            fars(step, (1,))
        side(3)
        mates(3)
        mine(4)
        side(4)
        fars(0, (2, 3))
        mate_panel(0)
        fars(1, (2, 3))
        mate_panel(1)
        mine(5)
        fars(2, (2, 3))
        mate_panel(2)
        mate_panel(3)

        def for_mate(step):
            first = (step == ahead).astype(jnp.int32)
            for turn_of in range(2):
                slot = first * (1 - turn_of) + (1 - first) * turn_of
                b = 2 * mate_z + slot * x + (1 - slot) * (1 - x)

                @pl.when(step == ahead)
                def _():
                    if turn_of == 1:
                        mates(step + 1)
                        side(step + 2)
                        mine(step + 3)
                        side(step + 3)
                        for q in range(nz):
                            panel_wait(mate_beside, q)
                            to_core(mate_beside, q).start()
                    core_wait((mate, mate_beside)[turn_of])
                    if turn_of == 1:
                        exchange(step + 5)
                        for q in range(1, nz):
                            panel(band, q, vec_side, beside).start()

                staged[step, slot] = product(step, b)

                @pl.when(slot == 0)
                def _():
                    for p in range(2):
                        to_pass(step, p).start()

                    @pl.when(step == steps - 1)
                    def _():
                        for p in range(2):
                            to_mate_out(step - 1, p).start()

                @pl.when((slot == 1) & (step < steps - 2))
                def _():
                    for p in range(2):
                        to_mate_out(step, p).start()

        def for_row(step, carry):
            staged[step, 2] = product(step, beside)
            for p in range(2):
                to_side_out(staged.at[step, 2, tile(p)], step, p).start()
            staged[step, 3] = product(step, band)
            keep(step).start()
            return carry

        lag = ahead + 3

        def rows_done(step):
            return jnp.minimum(jnp.maximum(step + 1 - lag, 0) * 5 // 3, steps)

        def body(step, carry):
            fars(step)
            for_mate(step)

            @pl.when(step + 2 < steps)
            def _():
                mates(step + 2)

            @pl.when((step > ahead) & (step + 3 < steps))
            def _():
                mine(step + 3)
                side(step + 3)

            @pl.when((step > ahead) & (step + 5 < steps))
            def _():
                exchange(step + 5)

            @pl.when(step == lag)
            def _():
                for q in range(nz):
                    panel_wait(beside, q)
                    to_core(beside, q).start()
                core_wait(band)
                core_wait(beside)

            lax.fori_loop(rows_done(step - 1), rows_done(step), for_row, 0)
            return carry

        lax.fori_loop(ahead, steps, body, 0)
        settle(parts.at[0, first_steps], sum_in.at[0])
        part[first_steps] = part[first_steps] + parts[0, first_steps]
        sum_to_peer().start()
        settle(parts.at[1], sum_in.at[1])
        halves[x] = (part[...] + parts[1]) / jnp.float32(total_bands)
        total_to(mate_beside, 3).start()
        total_to(mate, 2).start()
        total_to(beside, 3).start()
        for p in range(2):
            to_mate_out(steps - 1, p).start()

    @pl.when(outer)
    def _():
        def mine(step):
            own_ready(step)
            block(step, band, mate_out, mate, 1).start()

        def side(step):
            arrived(step, (beside,), 0)
            block(step, beside, mate_out, mate, 1).start()

        for step in range(ahead + 1):
            exchange(step)
            mine(step)
        lax.fori_loop(ahead + 1, steps, load, 0)
        turn()
        rest_ready()
        for step in range(ahead + 1, ahead + 5):
            exchange(step)
        for step in range(ahead + 1):
            side(step)
        for q in range(nz):
            panel(band, q, vec_mate, mate).start()
        for q in range(nz):
            panel(band, q, vec_side, beside).start()
            to_core(band, q).start()

        def begin(step, carry):
            exchange(step)
            return carry

        lax.fori_loop(ahead + 5, steps, begin, 0)
        weigh()
        for step in range(ahead + 1, ahead + 5):
            mine(step)
            side(step)
        for q in range(nz):
            panel_wait(beside, q)
            to_core(beside, q).start()
        core_wait(band)
        core_wait(beside)

        def shared(step, carry):
            for b in (mate, mate_beside, peer, peer_beside, far, far_beside):
                settle(gathered.at[step, b], early.at[step, b])
            staged[step, 2] = product(step, beside)
            for p in range(2):
                to_side_out(staged.at[step, 2, tile(p)], step, p).start()
            staged[step, 3] = product(step, band)
            keep(step).start()
            return carry

        lax.fori_loop(0, ahead, shared, 0)
        sum_to_mate().start()

        def body(step, carry):
            @pl.when(step + 5 < steps)
            def _():
                mine(step + 5)
                side(step + 5)

            settle(passing.at[step], pass_in.at[step - ahead])
            for p in range(2):
                to_side_out(passing.at[step, tile(p)], step, p).start()
            return carry

        lax.fori_loop(ahead, steps - 1, body, 0)
        for p in range(2):
            settle(passing.at[steps - 1, tile(p)], pass_in.at[steps - 1 - ahead + p])
            to_side_out(passing.at[steps - 1, tile(p)], steps - 1, p).start()

    @pl.when(outer)
    def _():
        settle(halves.at[x], sum_in.at[2])

    settle(halves.at[1 - x], sum_in.at[3])
    density[...] = halves[...]

    def blocks(n):
        return staged.at[pl.ds(0, n // 2), 0]

    settle(away, away_out.at[0])

    @pl.when(inner)
    def _():
        settle(gathered.at[pl.ds(0, steps // 2)], peer_out.at[0])
        settle(part, sum_out.at[0])
        settle(parts, sum_out.at[1])
        settle(blocks(6 * ahead), share_out.at[0])
        settle(vectors.at[:, pl.ds(0, 4 * width)], vec_core.at[0])
        settle(vectors.at[:, pl.ds(0, 2 * width)], vec_side.at[0])
        settle(staged.at[pl.ds(ahead, steps - ahead), pl.ds(0, 2)], res_mate.at[0])
        settle(blocks(2 * steps), kept.at[0])

    @pl.when(outer)
    def _():
        settle(part.at[first_steps], sum_out.at[0])
        settle(blocks(2 * steps), mate_out.at[0])
        settle(vectors.at[:, pl.ds(0, 2 * width)], vec_core.at[0])
        settle(vectors.at[:, pl.ds(0, width)], vec_side.at[0])
        settle(vectors.at[:, pl.ds(0, width)], vec_mate.at[0])
        settle(blocks(2 * ahead), kept.at[0])
        settle(blocks(2 * (steps - ahead)), mate_in.at[0])

    settle(blocks(2 * steps), side_out.at[0])
    settle(blocks(2 * steps), side_in.at[0])


def flush(rotated, density, rotated_out, density_out, sems):
    band = rotated.shape[0] // PIECES
    copies = [
        pltpu.make_async_copy(rotated.at[pl.ds(i * band, band)], rotated_out.at[pl.ds(i * band, band)], sems.at[i])
        for i in range(PIECES)
    ]
    copies.append(pltpu.make_async_copy(density, density_out, sems.at[PIECES]))
    for copy in copies:
        copy.start()
    for copy in copies:
        copy.wait()


def local(nb, wavefunctions, eigvec, occupation):
    rows, points = wavefunctions.shape
    total_bands, width = eigvec.shape
    steps = points // 2 // LANES
    if nb != 8 or width != LANES or rows != 2 * width or points % (2 * LANES) or steps < SHARED + 8 or total_bands != nb * rows:
        return plain(wavefunctions, eigvec, occupation)
    nz, deep = nb // 2, total_bands // (nb // 2)
    vmem = pl.BlockSpec(memory_space=pltpu.VMEM)
    hbm = pl.BlockSpec(memory_space=pltpu.HBM)
    dma = pltpu.SemaphoreType.DMA
    rotated, density = pl.pallas_call(
        kernel,
        out_shape=(
            pltpu.VMEM((rows, points), jnp.float32),
            pltpu.VMEM((2, steps, 1, LANES), jnp.float32),
        ),
        in_specs=[hbm] * 3,
        out_specs=(pl.BlockSpec(memory_space=pl.ANY), vmem),
        scratch_shapes=[
            pltpu.VMEM((steps, nb, rows, LANES), jnp.bfloat16),
            pltpu.VMEM((steps, rows, LANES), jnp.bfloat16),
            pltpu.VMEM((total_bands, width), jnp.bfloat16),
            pltpu.VMEM((nz, 4 * rows, deep), jnp.bfloat16),
            pltpu.VMEM((total_bands // LANES, LANES), jnp.float32),
            pltpu.VMEM((4 * rows, LANES), jnp.float32),
            pltpu.VMEM((steps, 4, rows, LANES), jnp.float32),
            pltpu.VMEM((steps, rows, LANES), jnp.float32),
            pltpu.VMEM((steps, 1, LANES), jnp.float32),
            pltpu.VMEM((3, steps, 1, LANES), jnp.float32),
            pltpu.VMEM((2, steps, 1, LANES), jnp.float32),
            dma((SHARED + 2,)),
            dma((SHARED + 2,)),
            dma((1,)),
            dma((1,)),
            dma((SHARED, nb)),
            dma((steps - SHARED, 3)),
            *[dma((1,))] * 4,
            dma((4, nz)),
            dma((4,)),
            *[dma((1,))] * 4,
            dma((steps - SHARED + 1,)),
            *[dma((1,))] * 4,
            dma((2,)),
            dma((4,)),
        ],
        compiler_params=pltpu.CompilerParams(
            collective_id=0, has_side_effects=True, vmem_limit_bytes=56 * 2**20
        ),
    )(wavefunctions, eigvec, occupation.reshape(total_bands // LANES, LANES))
    rotated, density = pl.pallas_call(
        flush,
        out_shape=(
            jax.ShapeDtypeStruct(rotated.shape, rotated.dtype),
            jax.ShapeDtypeStruct(density.shape, density.dtype),
        ),
        in_specs=[pl.BlockSpec(memory_space=pl.ANY)] * 2,
        out_specs=(hbm, hbm),
        scratch_shapes=[dma((PIECES + 1,))],
        compiler_params=pltpu.CompilerParams(vmem_limit_bytes=2**20),
    )(rotated, density)
    return (rotated, density.reshape(points))


def solution(mesh):
    placed = (P("band", ("frag", "slab")), P(None, ("frag", "band", "slab")), P("frag"))
    return jax.shard_map(
        functools.partial(local, mesh.shape["band"]),
        mesh=mesh,
        in_specs=placed,
        out_specs=(P("band", ("frag", "slab")), P(("frag", "slab"))),
        check_vma=False,
    )
```

```python
import functools

import jax
import jax.numpy as jnp
from jax import lax
from jax.experimental import pallas as pl
from jax.experimental.pallas import tpu as pltpu
from jax.sharding import PartitionSpec as P

MESH = pl.DeviceIdType.MESH
LANES = 128
PIECES = 8
SHARED = 3


def plain(wavefunctions, eigvec, occupation):
    total_bands = eigvec.shape[0]
    by_points = lax.all_to_all(wavefunctions, "band", split_axis=1, concat_axis=0, tiled=True)
    point_rows = lax.dot_general(
        lax.all_gather(eigvec, ("band", "slab"), axis=1, tiled=True),
        by_points,
        (((0,), (0,)), ((), ())),
        preferred_element_type=jnp.float32,
    )
    rotated = lax.all_to_all(point_rows, "band", split_axis=0, concat_axis=1, tiled=True)
    local_density = jnp.dot(
        occupation,
        point_rows * point_rows,
        precision=lax.Precision.HIGHEST,
        preferred_element_type=jnp.float32,
    ) / jnp.float32(total_bands)
    density = lax.all_gather(local_density, "band", axis=0, tiled=True)
    return (rotated, density)


def kernel(
    wave, eigvec, occupation, out, density,
    gathered, away, raw, vectors, seats, weight, staged, passing, part, parts, halves,
    own_in, away_in, raw_in, seats_in, early, late, away_out, peer_out, mate_out, share_out,
    vec_in, vec_core_in, vec_core, vec_side, vec_mate, res_mate, pass_in, mate_in, side_in, side_out, kept, sum_out, sum_in,
):
    nb, nz = gathered.shape[1], gathered.shape[1] // 2
    frag, band, slab = (lax.axis_index(name) for name in ("frag", "band", "slab"))
    z, x = band // 2, lax.rem(band, 2)
    end = z // 2
    inner = (z == 1) | (z == 2)
    outer = (z == 0) | (z == 3)
    rows, points = wave.shape
    half = points // 2
    steps = half // LANES
    total_bands, width = eigvec.shape
    deep = total_bands // nz
    tall = rows // 2
    ahead = SHARED

    mate_z = 4 * end + 1 - z
    beside = band + 1 - 2 * x
    mate, mate_beside = 2 * mate_z + x, 2 * mate_z + 1 - x
    peer, peer_beside = 2 * (3 - z) + x, 2 * (3 - z) + 1 - x
    far, far_beside = 2 * (3 - mate_z) + x, 2 * (3 - mate_z) + 1 - x

    def at(b, s=slab):
        return (frag, b, s)

    def send(src, dst, ssem, rsem, target):
        return pltpu.make_async_remote_copy(
            src_ref=src, dst_ref=dst, send_sem=ssem, recv_sem=rsem, device_id=target, device_id_type=MESH
        )

    def columns(of, step):
        return pl.ds(pl.multiple_of(of * half + step * LANES, LANES), LANES)

    def settle(ref, sem):
        pltpu.make_async_copy(ref, ref, sem).wait()

    def own_load(step, i):
        return pltpu.make_async_copy(wave.at[:, columns(x, step)], gathered.at[step, band], own_in.at[i])

    def away_load(step, i):
        return pltpu.make_async_copy(wave.at[:, columns(1 - x, step)], away.at[step], away_in.at[i])

    raw_load = pltpu.make_async_copy(eigvec, raw, raw_in.at[0])
    seats_load = pltpu.make_async_copy(occupation, seats, seats_in.at[0])

    def block(step, b, sem, target, way):
        there = gathered.at[step, b]
        rsem = early.at[step, b] if isinstance(step, int) and step < ahead else late.at[step - ahead, way]
        return send(there, there, sem.at[0], rsem, at(target))

    def across(step):
        rsem = early.at[step, band] if isinstance(step, int) and step < ahead else late.at[step - ahead, 0]
        return send(away.at[step], gathered.at[step, band], away_out.at[0], rsem, at(beside))

    def arrived(step, bands, way):
        if isinstance(step, int) and step < ahead:
            for b in bands:
                settle(gathered.at[step, b], early.at[step, b])
        else:
            settle(gathered.at[step, pl.ds(0, len(bands))], late.at[step - ahead, way])

    def seat_of(b):
        return b - 4 * end

    def panel_at(b, s):
        return pl.ds(pl.multiple_of((seat_of(b) * 2 + s) * width, width), width)

    def to_core(b, q):
        there = vectors.at[q, panel_at(b, slab)]
        return send(there, there, vec_core.at[0], vec_core_in.at[seat_of(b)], at(band, 1 - slab))

    def panel(b, q, sem, target):
        there = vectors.at[q, panel_at(b, slab)]
        return send(there, there, sem.at[0], vec_in.at[seat_of(b), q], at(target))

    def panel_wait(b, q):
        settle(vectors.at[q, panel_at(b, slab)], vec_in.at[seat_of(b), q])

    def core_wait(b):
        settle(vectors.at[:, panel_at(b, 1 - slab)], vec_core_in.at[seat_of(b)])

    def tile(p):
        return pl.ds(p * tall, tall)

    def pass_sem(step, p):
        return pass_in.at[step - ahead + p * (step == steps - 1)]

    def to_pass(step, p):
        return send(staged.at[step, 0, tile(p)], passing.at[step, tile(p)], res_mate.at[0], pass_sem(step, p), at(mate))

    def to_mate_out(step, p):
        there = out.at[tile(p), columns(x, step)]
        return send(staged.at[step, 1, tile(p)], there, res_mate.at[0], mate_in.at[0], at(mate))

    def to_side_out(src, step, p):
        return send(src, out.at[tile(p), columns(x, step)], side_out.at[0], side_in.at[0], at(beside))

    def keep(step):
        return pltpu.make_async_copy(staged.at[step, 3], out.at[:, columns(x, step)], kept.at[0])

    def product(step, b):
        first = pl.multiple_of(seat_of(b) * rows, rows)
        total = None
        for q in range(nz):
            term = jnp.dot(
                vectors[q, pl.ds(first, rows), :],
                gathered[step, pl.ds(2 * q, 2)].reshape(deep, LANES),
                preferred_element_type=jnp.float32,
            )
            total = term if total is None else total + term
        part[step] = part[step] + jnp.sum(weight[pl.ds(first, rows), :] * total * total, axis=0, keepdims=True)
        return total

    def load(step, carry):
        i = 0 if isinstance(step, int) else 1
        away_load(step, i).start()
        own_load(step, i).start()
        return carry

    barrier = pltpu.get_barrier_semaphore()
    for target in (at(beside), at(mate), at(band, 1 - slab)):
        pl.semaphore_signal(barrier, inc=1, device_id=target, device_id_type=MESH)

    @pl.when(inner)
    def _():
        pl.semaphore_signal(barrier, inc=1, device_id=at(peer), device_id_type=MESH)

    for step in range(ahead + 1):
        load(step, None)
    raw_load.start()
    seats_load.start()

    @pl.when(inner)
    def _():
        pl.semaphore_wait(barrier, 4)

    @pl.when(outer)
    def _():
        pl.semaphore_wait(barrier, 3)

    def exchange(step):
        across(step).start()

    def loaded(i):
        some = pl.ds(*((0, ahead + 1), (ahead + 1, steps - ahead - 1))[i])
        settle(away.at[some], away_in.at[i])
        settle(away.at[some], own_in.at[i])

    def turn():
        raw_load.wait()
        for q in range(nz):
            vectors[q, panel_at(band, slab), :] = raw[pl.ds(q * deep, deep), :].T

    def weigh():
        seats_load.wait()
        for group in range(8):
            row = seats[pl.ds(pl.multiple_of(8 * end, 8), 8), :][group : group + 1, :]
            weight[pl.ds(group * LANES, LANES), :] = jnp.broadcast_to(row, (LANES, LANES)).T

    part[...] = jnp.zeros(part.shape, part.dtype)

    first_steps = pl.ds(0, ahead)

    def sum_to_mate():
        return send(part.at[first_steps], parts.at[0, first_steps], sum_out.at[0], sum_in.at[0], at(mate))

    def sum_to_peer():
        return send(part, parts.at[1], sum_out.at[0], sum_in.at[1], at(peer))

    def total_to(b, i):
        return send(halves.at[x], halves.at[x], sum_out.at[1], sum_in.at[i], at(b))

    @pl.when(inner)
    def _():
        def onward(step, b):
            block(step, b, peer_out, peer, 2).start()

        def share(step, b):
            if isinstance(step, int) and step < ahead:
                block(step, b, share_out, mate, 1).start()

        def mine(step):
            onward(step, band)
            share(step, band)

        def side(step):
            arrived(step, (beside,), 0)
            onward(step, beside)
            share(step, beside)

        def mates(step, which=(0, 1)):
            bands = [(mate, mate_beside)[i] for i in which]
            arrived(step, bands, 1)
            for b in bands:
                onward(step, b)

        def fars(step, which=(0, 1, 2, 3)):
            bands = [(peer, peer_beside, far, far_beside)[i] for i in which]
            arrived(step, bands, 2)
            for b in bands:
                share(step, b)

        def mate_panel(q):
            panel_wait(mate, q)
            panel(mate, q, vec_side, beside).start()
            to_core(mate, q).start()

        loaded(0)
        for step in range(ahead):
            mine(step)
            exchange(step)
        exchange(ahead)
        lax.fori_loop(ahead + 1, steps, load, 0)
        turn()
        for q in range(nz):
            to_core(band, q).start()
        loaded(1)
        for step in range(4, 8):
            exchange(step)
        panel(band, 0, vec_side, beside).start()
        weigh()
        for step in range(ahead):
            side(step)
            mates(step, (0,))
            fars(step, (0,))
        mine(3)
        for step in range(ahead):
            mates(step, (1,))
            fars(step, (1,))
        side(3)
        mates(3)
        mine(4)
        side(4)
        fars(0, (2, 3))
        mate_panel(0)
        fars(1, (2, 3))
        mate_panel(1)
        mine(5)
        fars(2, (2, 3))
        mate_panel(2)
        mate_panel(3)

        def for_mate(step):
            first = (step == ahead).astype(jnp.int32)
            for turn_of in range(2):
                slot = first * (1 - turn_of) + (1 - first) * turn_of
                b = 2 * mate_z + slot * x + (1 - slot) * (1 - x)

                @pl.when(step == ahead)
                def _():
                    if turn_of == 1:
                        mates(step + 1)
                        side(step + 2)
                        mine(step + 3)
                        side(step + 3)
                        for q in range(nz):
                            panel_wait(mate_beside, q)
                            to_core(mate_beside, q).start()
                    core_wait((mate, mate_beside)[turn_of])
                    if turn_of == 1:
                        exchange(step + 5)
                        for q in range(1, nz):
                            panel(band, q, vec_side, beside).start()

                staged[step, slot] = product(step, b)

                @pl.when(slot == 0)
                def _():
                    for p in range(2):
                        to_pass(step, p).start()

                    @pl.when(step == steps - 1)
                    def _():
                        for p in range(2):
                            to_mate_out(step - 1, p).start()

                @pl.when((slot == 1) & (step < steps - 2))
                def _():
                    for p in range(2):
                        to_mate_out(step, p).start()

        def for_row(step, carry):
            staged[step, 2] = product(step, beside)
            for p in range(2):
                to_side_out(staged.at[step, 2, tile(p)], step, p).start()
            staged[step, 3] = product(step, band)
            keep(step).start()
            return carry

        lag = ahead + 3

        def rows_done(step):
            return jnp.minimum(jnp.maximum(step + 1 - lag, 0) * 5 // 3, steps)

        def body(step, carry):
            fars(step)
            for_mate(step)

            @pl.when(step + 2 < steps)
            def _():
                mates(step + 2)

            @pl.when((step > ahead) & (step + 3 < steps))
            def _():
                mine(step + 3)
                side(step + 3)

            @pl.when((step > ahead) & (step + 5 < steps))
            def _():
                exchange(step + 5)

            @pl.when(step == lag)
            def _():
                for q in range(nz):
                    panel_wait(beside, q)
                    to_core(beside, q).start()
                core_wait(band)
                core_wait(beside)

            lax.fori_loop(rows_done(step - 1), rows_done(step), for_row, 0)
            return carry

        lax.fori_loop(ahead, steps, body, 0)
        settle(parts.at[0, first_steps], sum_in.at[0])
        part[first_steps] = part[first_steps] + parts[0, first_steps]
        sum_to_peer().start()
        settle(parts.at[1], sum_in.at[1])
        halves[x] = (part[...] + parts[1]) / jnp.float32(total_bands)
        total_to(mate_beside, 3).start()
        total_to(mate, 2).start()
        total_to(beside, 3).start()
        for p in range(2):
            to_mate_out(steps - 1, p).start()

    @pl.when(outer)
    def _():
        def mine(step):
            block(step, band, mate_out, mate, 1).start()

        def side(step):
            arrived(step, (beside,), 0)
            block(step, beside, mate_out, mate, 1).start()

        loaded(0)
        for step in range(ahead + 1):
            exchange(step)
            mine(step)
        lax.fori_loop(ahead + 1, steps, load, 0)
        turn()
        loaded(1)
        for step in range(ahead + 1, ahead + 5):
            exchange(step)
        for step in range(ahead + 1):
            side(step)
        for q in range(nz):
            panel(band, q, vec_mate, mate).start()
        for q in range(nz):
            panel(band, q, vec_side, beside).start()
            to_core(band, q).start()

        def begin(step, carry):
            exchange(step)
            return carry

        lax.fori_loop(ahead + 5, steps, begin, 0)
        weigh()
        for step in range(ahead + 1, ahead + 5):
            mine(step)
            side(step)
        for q in range(nz):
            panel_wait(beside, q)
            to_core(beside, q).start()
        core_wait(band)
        core_wait(beside)

        def shared(step, carry):
            for b in (mate, mate_beside, peer, peer_beside, far, far_beside):
                settle(gathered.at[step, b], early.at[step, b])
            staged[step, 2] = product(step, beside)
            for p in range(2):
                to_side_out(staged.at[step, 2, tile(p)], step, p).start()
            staged[step, 3] = product(step, band)
            keep(step).start()
            return carry

        lax.fori_loop(0, ahead, shared, 0)
        sum_to_mate().start()

        def body(step, carry):
            @pl.when(step + 5 < steps)
            def _():
                mine(step + 5)
                side(step + 5)

            settle(passing.at[step], pass_in.at[step - ahead])
            for p in range(2):
                to_side_out(passing.at[step, tile(p)], step, p).start()
            return carry

        lax.fori_loop(ahead, steps - 1, body, 0)
        for p in range(2):
            settle(passing.at[steps - 1, tile(p)], pass_in.at[steps - 1 - ahead + p])
            to_side_out(passing.at[steps - 1, tile(p)], steps - 1, p).start()

    @pl.when(outer)
    def _():
        settle(halves.at[x], sum_in.at[2])

    settle(halves.at[1 - x], sum_in.at[3])
    density[...] = halves[...]

    def blocks(n):
        return staged.at[pl.ds(0, n // 2), 0]

    settle(away, away_out.at[0])

    @pl.when(inner)
    def _():
        settle(gathered.at[pl.ds(0, steps // 2)], peer_out.at[0])
        settle(part, sum_out.at[0])
        settle(parts, sum_out.at[1])
        settle(blocks(6 * ahead), share_out.at[0])
        settle(vectors.at[:, pl.ds(0, 4 * width)], vec_core.at[0])
        settle(vectors.at[:, pl.ds(0, 2 * width)], vec_side.at[0])
        settle(staged.at[pl.ds(ahead, steps - ahead), pl.ds(0, 2)], res_mate.at[0])
        settle(blocks(2 * steps), kept.at[0])

    @pl.when(outer)
    def _():
        settle(part.at[first_steps], sum_out.at[0])
        settle(blocks(2 * steps), mate_out.at[0])
        settle(vectors.at[:, pl.ds(0, 2 * width)], vec_core.at[0])
        settle(vectors.at[:, pl.ds(0, width)], vec_side.at[0])
        settle(vectors.at[:, pl.ds(0, width)], vec_mate.at[0])
        settle(blocks(2 * ahead), kept.at[0])
        settle(blocks(2 * (steps - ahead)), mate_in.at[0])

    settle(blocks(2 * steps), side_out.at[0])
    settle(blocks(2 * steps), side_in.at[0])


def flush(rotated, density, rotated_out, density_out, sems):
    band = rotated.shape[0] // PIECES
    copies = [
        pltpu.make_async_copy(rotated.at[pl.ds(i * band, band)], rotated_out.at[pl.ds(i * band, band)], sems.at[i])
        for i in range(PIECES)
    ]
    copies.append(pltpu.make_async_copy(density, density_out, sems.at[PIECES]))
    for copy in copies:
        copy.start()
    for copy in copies:
        copy.wait()


def local(nb, wavefunctions, eigvec, occupation):
    rows, points = wavefunctions.shape
    total_bands, width = eigvec.shape
    steps = points // 2 // LANES
    if nb != 8 or width != LANES or rows != 2 * width or points % (2 * LANES) or steps < SHARED + 8 or total_bands != nb * rows:
        return plain(wavefunctions, eigvec, occupation)
    nz, deep = nb // 2, total_bands // (nb // 2)
    vmem = pl.BlockSpec(memory_space=pltpu.VMEM)
    hbm = pl.BlockSpec(memory_space=pltpu.HBM)
    dma = pltpu.SemaphoreType.DMA
    rotated, density = pl.pallas_call(
        kernel,
        out_shape=(
            pltpu.VMEM((rows, points), jnp.float32),
            pltpu.VMEM((2, steps, 1, LANES), jnp.float32),
        ),
        in_specs=[hbm] * 3,
        out_specs=(pl.BlockSpec(memory_space=pl.ANY), vmem),
        scratch_shapes=[
            pltpu.VMEM((steps, nb, rows, LANES), jnp.bfloat16),
            pltpu.VMEM((steps, rows, LANES), jnp.bfloat16),
            pltpu.VMEM((total_bands, width), jnp.bfloat16),
            pltpu.VMEM((nz, 4 * rows, deep), jnp.bfloat16),
            pltpu.VMEM((total_bands // LANES, LANES), jnp.float32),
            pltpu.VMEM((4 * rows, LANES), jnp.float32),
            pltpu.VMEM((steps, 4, rows, LANES), jnp.float32),
            pltpu.VMEM((steps, rows, LANES), jnp.float32),
            pltpu.VMEM((steps, 1, LANES), jnp.float32),
            pltpu.VMEM((3, steps, 1, LANES), jnp.float32),
            pltpu.VMEM((2, steps, 1, LANES), jnp.float32),
            dma((2,)),
            dma((2,)),
            dma((1,)),
            dma((1,)),
            dma((SHARED, nb)),
            dma((steps - SHARED, 3)),
            *[dma((1,))] * 4,
            dma((4, nz)),
            dma((4,)),
            *[dma((1,))] * 4,
            dma((steps - SHARED + 1,)),
            *[dma((1,))] * 4,
            dma((2,)),
            dma((4,)),
        ],
        compiler_params=pltpu.CompilerParams(
            collective_id=0, has_side_effects=True, vmem_limit_bytes=56 * 2**20
        ),
    )(wavefunctions, eigvec, occupation.reshape(total_bands // LANES, LANES))
    rotated, density = pl.pallas_call(
        flush,
        out_shape=(
            jax.ShapeDtypeStruct(rotated.shape, rotated.dtype),
            jax.ShapeDtypeStruct(density.shape, density.dtype),
        ),
        in_specs=[pl.BlockSpec(memory_space=pl.ANY)] * 2,
        out_specs=(hbm, hbm),
        scratch_shapes=[dma((PIECES + 1,))],
        compiler_params=pltpu.CompilerParams(vmem_limit_bytes=2**20),
    )(rotated, density)
    return (rotated, density.reshape(points))


def solution(mesh):
    placed = (P("band", ("frag", "slab")), P(None, ("frag", "band", "slab")), P("frag"))
    return jax.shard_map(
        functools.partial(local, mesh.shape["band"]),
        mesh=mesh,
        in_specs=placed,
        out_specs=(P("band", ("frag", "slab")), P(("frag", "slab"))),
        check_vma=False,
    )
```

```python
import functools

import jax
import jax.numpy as jnp
from jax import lax
from jax.experimental import pallas as pl
from jax.experimental.pallas import tpu as pltpu
from jax.sharding import PartitionSpec as P

MESH = pl.DeviceIdType.MESH
LANES = 128
PIECES = 2
SHARED = 3


def plain(wavefunctions, eigvec, occupation):
    total_bands = eigvec.shape[0]
    by_points = lax.all_to_all(wavefunctions, "band", split_axis=1, concat_axis=0, tiled=True)
    point_rows = lax.dot_general(
        lax.all_gather(eigvec, ("band", "slab"), axis=1, tiled=True),
        by_points,
        (((0,), (0,)), ((), ())),
        preferred_element_type=jnp.float32,
    )
    rotated = lax.all_to_all(point_rows, "band", split_axis=0, concat_axis=1, tiled=True)
    local_density = jnp.dot(
        occupation,
        point_rows * point_rows,
        precision=lax.Precision.HIGHEST,
        preferred_element_type=jnp.float32,
    ) / jnp.float32(total_bands)
    density = lax.all_gather(local_density, "band", axis=0, tiled=True)
    return (rotated, density)


def kernel(
    wave, eigvec, occupation, out, density,
    gathered, away, raw, vectors, seats, weight, staged, passing, part, parts, halves,
    own_in, away_in, raw_in, seats_in, early, late, away_out, peer_out, mate_out, share_out,
    vec_in, vec_core_in, vec_core, vec_side, vec_mate, res_mate, pass_in, mate_in, side_in, side_out, kept, sum_out, sum_in,
):
    nb, nz = gathered.shape[1], gathered.shape[1] // 2
    frag, band, slab = (lax.axis_index(name) for name in ("frag", "band", "slab"))
    z, x = band // 2, lax.rem(band, 2)
    end = z // 2
    inner = (z == 1) | (z == 2)
    outer = (z == 0) | (z == 3)
    rows, points = wave.shape
    half = points // 2
    steps = half // LANES
    total_bands, width = eigvec.shape
    deep = total_bands // nz
    tall = rows // 2
    ahead = SHARED

    mate_z = 4 * end + 1 - z
    beside = band + 1 - 2 * x
    mate, mate_beside = 2 * mate_z + x, 2 * mate_z + 1 - x
    peer, peer_beside = 2 * (3 - z) + x, 2 * (3 - z) + 1 - x
    far, far_beside = 2 * (3 - mate_z) + x, 2 * (3 - mate_z) + 1 - x

    def at(b, s=slab):
        return (frag, b, s)

    def send(src, dst, ssem, rsem, target):
        return pltpu.make_async_remote_copy(
            src_ref=src, dst_ref=dst, send_sem=ssem, recv_sem=rsem, device_id=target, device_id_type=MESH
        )

    def columns(of, step):
        return pl.ds(pl.multiple_of(of * half + step * LANES, LANES), LANES)

    def settle(ref, sem):
        pltpu.make_async_copy(ref, ref, sem).wait()

    def own_load(step, i):
        return pltpu.make_async_copy(wave.at[:, columns(x, step)], gathered.at[step, band], own_in.at[i])

    def away_load(step, i):
        return pltpu.make_async_copy(wave.at[:, columns(1 - x, step)], away.at[step], away_in.at[i])

    raw_load = pltpu.make_async_copy(eigvec, raw, raw_in.at[0])
    seats_load = pltpu.make_async_copy(occupation, seats, seats_in.at[0])

    def block(step, b, sem, target, way):
        there = gathered.at[step, b]
        rsem = early.at[step, b] if isinstance(step, int) and step < ahead else late.at[step - ahead, way]
        return send(there, there, sem.at[0], rsem, at(target))

    def across(step):
        rsem = early.at[step, band] if isinstance(step, int) and step < ahead else late.at[step - ahead, 0]
        return send(away.at[step], gathered.at[step, band], away_out.at[0], rsem, at(beside))

    def arrived(step, bands, way):
        if isinstance(step, int) and step < ahead:
            for b in bands:
                settle(gathered.at[step, b], early.at[step, b])
        else:
            settle(gathered.at[step, pl.ds(0, len(bands))], late.at[step - ahead, way])

    def seat_of(b):
        return b - 4 * end

    def panel_at(b, s):
        return pl.ds(pl.multiple_of((seat_of(b) * 2 + s) * width, width), width)

    def to_core(b, q):
        there = vectors.at[q, panel_at(b, slab)]
        return send(there, there, vec_core.at[0], vec_core_in.at[seat_of(b)], at(band, 1 - slab))

    def panel(b, q, sem, target):
        there = vectors.at[q, panel_at(b, slab)]
        return send(there, there, sem.at[0], vec_in.at[seat_of(b), q], at(target))

    def panel_wait(b, q):
        settle(vectors.at[q, panel_at(b, slab)], vec_in.at[seat_of(b), q])

    def core_wait(b):
        settle(vectors.at[:, panel_at(b, 1 - slab)], vec_core_in.at[seat_of(b)])

    def tile(p):
        return pl.ds(p * tall, tall)

    def pass_sem(step, p):
        return pass_in.at[step - ahead + p * (step == steps - 1)]

    def to_pass(step, p):
        return send(staged.at[step, 0, tile(p)], passing.at[step, tile(p)], res_mate.at[0], pass_sem(step, p), at(mate))

    def to_mate_out(step, p):
        there = out.at[tile(p), columns(x, step)]
        return send(staged.at[step, 1, tile(p)], there, res_mate.at[0], mate_in.at[0], at(mate))

    def to_side_out(src, step, p):
        return send(src, out.at[tile(p), columns(x, step)], side_out.at[0], side_in.at[0], at(beside))

    def keep(step):
        return pltpu.make_async_copy(staged.at[step, 3], out.at[:, columns(x, step)], kept.at[0])

    def product(step, b):
        first = pl.multiple_of(seat_of(b) * rows, rows)
        total = None
        for q in range(nz):
            term = jnp.dot(
                vectors[q, pl.ds(first, rows), :],
                gathered[step, pl.ds(2 * q, 2)].reshape(deep, LANES),
                preferred_element_type=jnp.float32,
            )
            total = term if total is None else total + term
        part[step] = part[step] + jnp.sum(weight[pl.ds(first, rows), :] * total * total, axis=0, keepdims=True)
        return total

    def load(step, carry):
        i = 0 if isinstance(step, int) else 1
        away_load(step, i).start()
        own_load(step, i).start()
        return carry

    barrier = pltpu.get_barrier_semaphore()
    for target in (at(beside), at(mate), at(band, 1 - slab)):
        pl.semaphore_signal(barrier, inc=1, device_id=target, device_id_type=MESH)

    @pl.when(inner)
    def _():
        pl.semaphore_signal(barrier, inc=1, device_id=at(peer), device_id_type=MESH)

    for step in range(ahead + 1):
        load(step, None)
    raw_load.start()
    seats_load.start()

    @pl.when(inner)
    def _():
        pl.semaphore_wait(barrier, 4)

    @pl.when(outer)
    def _():
        pl.semaphore_wait(barrier, 3)

    def exchange(step):
        across(step).start()

    def loaded(i):
        some = pl.ds(*((0, ahead + 1), (ahead + 1, steps - ahead - 1))[i])
        settle(away.at[some], away_in.at[i])
        settle(away.at[some], own_in.at[i])

    def turn():
        raw_load.wait()
        for q in range(nz):
            vectors[q, panel_at(band, slab), :] = raw[pl.ds(q * deep, deep), :].T

    def weigh():
        seats_load.wait()
        for group in range(8):
            row = seats[pl.ds(pl.multiple_of(8 * end, 8), 8), :][group : group + 1, :]
            weight[pl.ds(group * LANES, LANES), :] = jnp.broadcast_to(row, (LANES, LANES)).T

    part[...] = jnp.zeros(part.shape, part.dtype)

    first_steps = pl.ds(0, ahead)

    def sum_to_mate():
        return send(part.at[first_steps], parts.at[0, first_steps], sum_out.at[0], sum_in.at[0], at(mate))

    def sum_to_peer():
        return send(part, parts.at[1], sum_out.at[0], sum_in.at[1], at(peer))

    def total_to(b, i):
        return send(halves.at[x], halves.at[x], sum_out.at[1], sum_in.at[i], at(b))

    @pl.when(inner)
    def _():
        def onward(step, b):
            block(step, b, peer_out, peer, 2).start()

        def share(step, b):
            if isinstance(step, int) and step < ahead:
                block(step, b, share_out, mate, 1).start()

        def mine(step):
            onward(step, band)
            share(step, band)

        def side(step):
            arrived(step, (beside,), 0)
            onward(step, beside)
            share(step, beside)

        def mates(step, which=(0, 1)):
            bands = [(mate, mate_beside)[i] for i in which]
            arrived(step, bands, 1)
            for b in bands:
                onward(step, b)

        def fars(step, which=(0, 1, 2, 3)):
            bands = [(peer, peer_beside, far, far_beside)[i] for i in which]
            arrived(step, bands, 2)
            for b in bands:
                share(step, b)

        def mate_panel(q):
            panel_wait(mate, q)
            panel(mate, q, vec_side, beside).start()
            to_core(mate, q).start()

        loaded(0)
        for step in range(ahead):
            mine(step)
            exchange(step)
        exchange(ahead)
        lax.fori_loop(ahead + 1, steps, load, 0)
        turn()
        for q in range(nz):
            to_core(band, q).start()
        loaded(1)
        for step in range(4, 8):
            exchange(step)
        panel(band, 0, vec_side, beside).start()
        weigh()
        for step in range(ahead):
            side(step)
            mates(step, (0,))
            fars(step, (0,))
        mine(3)
        for step in range(ahead):
            mates(step, (1,))
            fars(step, (1,))
        side(3)
        mates(3)
        mine(4)
        side(4)
        fars(0, (2, 3))
        mate_panel(0)
        fars(1, (2, 3))
        mate_panel(1)
        mine(5)
        fars(2, (2, 3))
        mate_panel(2)
        mate_panel(3)

        def for_mate(step):
            first = (step == ahead).astype(jnp.int32)
            for turn_of in range(2):
                slot = first * (1 - turn_of) + (1 - first) * turn_of
                b = 2 * mate_z + slot * x + (1 - slot) * (1 - x)

                @pl.when(step == ahead)
                def _():
                    if turn_of == 1:
                        mates(step + 1)
                        side(step + 2)
                        mine(step + 3)
                        side(step + 3)
                        for q in range(nz):
                            panel_wait(mate_beside, q)
                            to_core(mate_beside, q).start()
                    core_wait((mate, mate_beside)[turn_of])
                    if turn_of == 1:
                        exchange(step + 5)
                        for q in range(1, nz):
                            panel(band, q, vec_side, beside).start()

                staged[step, slot] = product(step, b)

                @pl.when(slot == 0)
                def _():
                    for p in range(2):
                        to_pass(step, p).start()

                    @pl.when(step == steps - 1)
                    def _():
                        for p in range(2):
                            to_mate_out(step - 1, p).start()

                @pl.when((slot == 1) & (step < steps - 2))
                def _():
                    for p in range(2):
                        to_mate_out(step, p).start()

        def for_row(step, carry):
            staged[step, 2] = product(step, beside)
            for p in range(2):
                to_side_out(staged.at[step, 2, tile(p)], step, p).start()
            staged[step, 3] = product(step, band)
            keep(step).start()
            return carry

        lag = ahead + 3

        def rows_done(step):
            return jnp.minimum(jnp.maximum(step + 1 - lag, 0) * 5 // 3, steps)

        def body(step, carry):
            fars(step)
            for_mate(step)

            @pl.when(step + 2 < steps)
            def _():
                mates(step + 2)

            @pl.when((step > ahead) & (step + 3 < steps))
            def _():
                mine(step + 3)
                side(step + 3)

            @pl.when((step > ahead) & (step + 5 < steps))
            def _():
                exchange(step + 5)

            @pl.when(step == lag)
            def _():
                for q in range(nz):
                    panel_wait(beside, q)
                    to_core(beside, q).start()
                core_wait(band)
                core_wait(beside)

            lax.fori_loop(rows_done(step - 1), rows_done(step), for_row, 0)
            return carry

        lax.fori_loop(ahead, steps, body, 0)
        settle(parts.at[0, first_steps], sum_in.at[0])
        part[first_steps] = part[first_steps] + parts[0, first_steps]
        sum_to_peer().start()
        settle(parts.at[1], sum_in.at[1])
        halves[x] = (part[...] + parts[1]) / jnp.float32(total_bands)
        total_to(mate_beside, 3).start()
        total_to(mate, 2).start()
        total_to(beside, 3).start()
        for p in range(2):
            to_mate_out(steps - 1, p).start()

    @pl.when(outer)
    def _():
        def mine(step):
            block(step, band, mate_out, mate, 1).start()

        def side(step):
            arrived(step, (beside,), 0)
            block(step, beside, mate_out, mate, 1).start()

        loaded(0)
        for step in range(ahead + 1):
            exchange(step)
            mine(step)
        lax.fori_loop(ahead + 1, steps, load, 0)
        turn()
        loaded(1)
        for step in range(ahead + 1, ahead + 5):
            exchange(step)
        for step in range(ahead + 1):
            side(step)
        for q in range(nz):
            panel(band, q, vec_mate, mate).start()
        for q in range(nz):
            panel(band, q, vec_side, beside).start()
            to_core(band, q).start()

        def begin(step, carry):
            exchange(step)
            return carry

        lax.fori_loop(ahead + 5, steps, begin, 0)
        weigh()
        for step in range(ahead + 1, ahead + 5):
            mine(step)
            side(step)
        for q in range(nz):
            panel_wait(beside, q)
            to_core(beside, q).start()
        core_wait(band)
        core_wait(beside)

        def shared(step, carry):
            for b in (mate, mate_beside, peer, peer_beside, far, far_beside):
                settle(gathered.at[step, b], early.at[step, b])
            staged[step, 2] = product(step, beside)
            for p in range(2):
                to_side_out(staged.at[step, 2, tile(p)], step, p).start()
            staged[step, 3] = product(step, band)
            keep(step).start()
            return carry

        lax.fori_loop(0, ahead, shared, 0)
        sum_to_mate().start()

        def body(step, carry):
            @pl.when(step + 5 < steps)
            def _():
                mine(step + 5)
                side(step + 5)

            settle(passing.at[step], pass_in.at[step - ahead])
            for p in range(2):
                to_side_out(passing.at[step, tile(p)], step, p).start()
            return carry

        lax.fori_loop(ahead, steps - 1, body, 0)
        for p in range(2):
            settle(passing.at[steps - 1, tile(p)], pass_in.at[steps - 1 - ahead + p])
            to_side_out(passing.at[steps - 1, tile(p)], steps - 1, p).start()

    @pl.when(outer)
    def _():
        settle(halves.at[x], sum_in.at[2])

    settle(halves.at[1 - x], sum_in.at[3])
    density[...] = halves[...]

    def blocks(n):
        return staged.at[pl.ds(0, n // 2), 0]

    settle(away, away_out.at[0])

    @pl.when(inner)
    def _():
        settle(gathered.at[pl.ds(0, steps // 2)], peer_out.at[0])
        settle(part, sum_out.at[0])
        settle(parts, sum_out.at[1])
        settle(blocks(6 * ahead), share_out.at[0])
        settle(vectors.at[:, pl.ds(0, 4 * width)], vec_core.at[0])
        settle(vectors.at[:, pl.ds(0, 2 * width)], vec_side.at[0])
        settle(staged.at[pl.ds(ahead, steps - ahead), pl.ds(0, 2)], res_mate.at[0])
        settle(blocks(2 * steps), kept.at[0])

    @pl.when(outer)
    def _():
        settle(part.at[first_steps], sum_out.at[0])
        settle(blocks(2 * steps), mate_out.at[0])
        settle(vectors.at[:, pl.ds(0, 2 * width)], vec_core.at[0])
        settle(vectors.at[:, pl.ds(0, width)], vec_side.at[0])
        settle(vectors.at[:, pl.ds(0, width)], vec_mate.at[0])
        settle(blocks(2 * ahead), kept.at[0])
        settle(blocks(2 * (steps - ahead)), mate_in.at[0])

    settle(blocks(2 * steps), side_out.at[0])
    settle(blocks(2 * steps), side_in.at[0])


def flush(rotated, density, rotated_out, density_out, sems):
    band = rotated.shape[0] // PIECES
    copies = [
        pltpu.make_async_copy(rotated.at[pl.ds(i * band, band)], rotated_out.at[pl.ds(i * band, band)], sems.at[i])
        for i in range(PIECES)
    ]
    copies.append(pltpu.make_async_copy(density, density_out, sems.at[PIECES]))
    for copy in copies:
        copy.start()
    for copy in copies:
        copy.wait()


def local(nb, wavefunctions, eigvec, occupation):
    rows, points = wavefunctions.shape
    total_bands, width = eigvec.shape
    steps = points // 2 // LANES
    if nb != 8 or width != LANES or rows != 2 * width or points % (2 * LANES) or steps < SHARED + 8 or total_bands != nb * rows:
        return plain(wavefunctions, eigvec, occupation)
    nz, deep = nb // 2, total_bands // (nb // 2)
    vmem = pl.BlockSpec(memory_space=pltpu.VMEM)
    hbm = pl.BlockSpec(memory_space=pltpu.HBM)
    dma = pltpu.SemaphoreType.DMA
    rotated, density = pl.pallas_call(
        kernel,
        out_shape=(
            pltpu.VMEM((rows, points), jnp.float32),
            pltpu.VMEM((2, steps, 1, LANES), jnp.float32),
        ),
        in_specs=[hbm] * 3,
        out_specs=(pl.BlockSpec(memory_space=pl.ANY), vmem),
        scratch_shapes=[
            pltpu.VMEM((steps, nb, rows, LANES), jnp.bfloat16),
            pltpu.VMEM((steps, rows, LANES), jnp.bfloat16),
            pltpu.VMEM((total_bands, width), jnp.bfloat16),
            pltpu.VMEM((nz, 4 * rows, deep), jnp.bfloat16),
            pltpu.VMEM((total_bands // LANES, LANES), jnp.float32),
            pltpu.VMEM((4 * rows, LANES), jnp.float32),
            pltpu.VMEM((steps, 4, rows, LANES), jnp.float32),
            pltpu.VMEM((steps, rows, LANES), jnp.float32),
            pltpu.VMEM((steps, 1, LANES), jnp.float32),
            pltpu.VMEM((3, steps, 1, LANES), jnp.float32),
            pltpu.VMEM((2, steps, 1, LANES), jnp.float32),
            dma((2,)),
            dma((2,)),
            dma((1,)),
            dma((1,)),
            dma((SHARED, nb)),
            dma((steps - SHARED, 3)),
            *[dma((1,))] * 4,
            dma((4, nz)),
            dma((4,)),
            *[dma((1,))] * 4,
            dma((steps - SHARED + 1,)),
            *[dma((1,))] * 4,
            dma((2,)),
            dma((4,)),
        ],
        compiler_params=pltpu.CompilerParams(
            collective_id=0, has_side_effects=True, vmem_limit_bytes=56 * 2**20
        ),
    )(wavefunctions, eigvec, occupation.reshape(total_bands // LANES, LANES))
    rotated, density = pl.pallas_call(
        flush,
        out_shape=(
            jax.ShapeDtypeStruct(rotated.shape, rotated.dtype),
            jax.ShapeDtypeStruct(density.shape, density.dtype),
        ),
        in_specs=[pl.BlockSpec(memory_space=pl.ANY)] * 2,
        out_specs=(hbm, hbm),
        scratch_shapes=[dma((PIECES + 1,))],
        compiler_params=pltpu.CompilerParams(vmem_limit_bytes=2**20),
    )(rotated, density)
    return (rotated, density.reshape(points))


def solution(mesh):
    placed = (P("band", ("frag", "slab")), P(None, ("frag", "band", "slab")), P("frag"))
    return jax.shard_map(
        functools.partial(local, mesh.shape["band"]),
        mesh=mesh,
        in_specs=placed,
        out_specs=(P("band", ("frag", "slab")), P(("frag", "slab"))),
        check_vma=False,
    )
```

```python
import functools

import jax
import jax.numpy as jnp
from jax import lax
from jax.experimental import pallas as pl
from jax.experimental.pallas import tpu as pltpu
from jax.sharding import PartitionSpec as P

MESH = pl.DeviceIdType.MESH
LANES = 128
PIECES = 2
SHARED = 3


def plain(wavefunctions, eigvec, occupation):
    total_bands = eigvec.shape[0]
    by_points = lax.all_to_all(wavefunctions, "band", split_axis=1, concat_axis=0, tiled=True)
    point_rows = lax.dot_general(
        lax.all_gather(eigvec, ("band", "slab"), axis=1, tiled=True),
        by_points,
        (((0,), (0,)), ((), ())),
        preferred_element_type=jnp.float32,
    )
    rotated = lax.all_to_all(point_rows, "band", split_axis=0, concat_axis=1, tiled=True)
    local_density = jnp.dot(
        occupation,
        point_rows * point_rows,
        precision=lax.Precision.HIGHEST,
        preferred_element_type=jnp.float32,
    ) / jnp.float32(total_bands)
    density = lax.all_gather(local_density, "band", axis=0, tiled=True)
    return (rotated, density)


def kernel(
    wave, eigvec, occupation, out, density,
    gathered, away, raw, vectors, seats, weight, staged, passing, part, parts, halves,
    own_in, away_in, raw_in, seats_in, early, late, away_out, peer_out, mate_out, share_out,
    vec_in, vec_core_in, vec_core, vec_side, vec_mate, res_mate, pass_in, mate_in, side_in, side_out, kept, sum_out, sum_in,
):
    nb, nz = gathered.shape[1], gathered.shape[1] // 2
    frag, band, slab = (lax.axis_index(name) for name in ("frag", "band", "slab"))
    z, x = band // 2, lax.rem(band, 2)
    end = z // 2
    inner = (z == 1) | (z == 2)
    outer = (z == 0) | (z == 3)
    rows, points = wave.shape
    half = points // 2
    steps = half // LANES
    total_bands, width = eigvec.shape
    deep = total_bands // nz
    tall = rows // 2
    ahead = SHARED

    mate_z = 4 * end + 1 - z
    beside = band + 1 - 2 * x
    mate, mate_beside = 2 * mate_z + x, 2 * mate_z + 1 - x
    peer, peer_beside = 2 * (3 - z) + x, 2 * (3 - z) + 1 - x
    far, far_beside = 2 * (3 - mate_z) + x, 2 * (3 - mate_z) + 1 - x

    def at(b, s=slab):
        return (frag, b, s)

    def send(src, dst, ssem, rsem, target):
        return pltpu.make_async_remote_copy(
            src_ref=src, dst_ref=dst, send_sem=ssem, recv_sem=rsem, device_id=target, device_id_type=MESH
        )

    def columns(of, step):
        return pl.ds(pl.multiple_of(of * half + step * LANES, LANES), LANES)

    def settle(ref, sem):
        pltpu.make_async_copy(ref, ref, sem).wait()

    def own_load(step, i):
        return pltpu.make_async_copy(wave.at[:, columns(x, step)], gathered.at[step, band], own_in.at[i])

    def away_load(step, i):
        return pltpu.make_async_copy(wave.at[:, columns(1 - x, step)], away.at[step], away_in.at[i])

    raw_load = pltpu.make_async_copy(eigvec, raw, raw_in.at[0])
    seats_load = pltpu.make_async_copy(occupation, seats, seats_in.at[0])

    def block(step, b, sem, target, way):
        there = gathered.at[step, b]
        rsem = early.at[step, b] if isinstance(step, int) and step < ahead else late.at[step - ahead, way]
        return send(there, there, sem.at[0], rsem, at(target))

    def across(step):
        rsem = early.at[step, band] if isinstance(step, int) and step < ahead else late.at[step - ahead, 0]
        return send(away.at[step], gathered.at[step, band], away_out.at[0], rsem, at(beside))

    def arrived(step, bands, way):
        if isinstance(step, int) and step < ahead:
            for b in bands:
                settle(gathered.at[step, b], early.at[step, b])
        else:
            settle(gathered.at[step, pl.ds(0, len(bands))], late.at[step - ahead, way])

    def seat_of(b):
        return b - 4 * end

    def panel_at(b, s):
        return pl.ds(pl.multiple_of((seat_of(b) * 2 + s) * width, width), width)

    def to_core(b, q):
        there = vectors.at[q, panel_at(b, slab)]
        return send(there, there, vec_core.at[0], vec_core_in.at[seat_of(b)], at(band, 1 - slab))

    def panel(b, q, sem, target):
        there = vectors.at[q, panel_at(b, slab)]
        return send(there, there, sem.at[0], vec_in.at[seat_of(b), q], at(target))

    def panel_wait(b, q):
        settle(vectors.at[q, panel_at(b, slab)], vec_in.at[seat_of(b), q])

    def core_wait(b):
        settle(vectors.at[:, panel_at(b, 1 - slab)], vec_core_in.at[seat_of(b)])

    def tile(p):
        return pl.ds(p * tall, tall)

    def pass_sem(step, p):
        return pass_in.at[step - ahead + p * (step == steps - 1)]

    def to_pass(step, p):
        return send(staged.at[step, 0, tile(p)], passing.at[step, tile(p)], res_mate.at[0], pass_sem(step, p), at(mate))

    def to_mate_out(step, p):
        there = out.at[tile(p), columns(x, step)]
        return send(staged.at[step, 1, tile(p)], there, res_mate.at[0], mate_in.at[0], at(mate))

    def to_side_out(src, step, p):
        return send(src, out.at[tile(p), columns(x, step)], side_out.at[0], side_in.at[0], at(beside))

    def keep(step):
        return pltpu.make_async_copy(staged.at[step, 3], out.at[:, columns(x, step)], kept.at[0])

    def product(step, b):
        first = pl.multiple_of(seat_of(b) * rows, rows)
        total = None
        for q in range(nz):
            term = jnp.dot(
                vectors[q, pl.ds(first, rows), :],
                gathered[step, pl.ds(2 * q, 2)].reshape(deep, LANES),
                preferred_element_type=jnp.float32,
            )
            total = term if total is None else total + term
        part[step] = part[step] + jnp.sum(weight[pl.ds(first, rows), :] * total * total, axis=0, keepdims=True)
        return total

    def load(step, carry):
        i = 0 if isinstance(step, int) else 1
        away_load(step, i).start()
        own_load(step, i).start()
        return carry

    barrier = pltpu.get_barrier_semaphore()
    for target in (at(beside), at(mate), at(band, 1 - slab)):
        pl.semaphore_signal(barrier, inc=1, device_id=target, device_id_type=MESH)

    @pl.when(inner)
    def _():
        pl.semaphore_signal(barrier, inc=1, device_id=at(peer), device_id_type=MESH)

    for step in range(ahead + 1):
        load(step, None)
    raw_load.start()
    seats_load.start()

    @pl.when(inner)
    def _():
        pl.semaphore_wait(barrier, 4)

    @pl.when(outer)
    def _():
        pl.semaphore_wait(barrier, 3)

    def exchange(step):
        across(step).start()

    def loaded(i):
        some = pl.ds(*((0, ahead + 1), (ahead + 1, steps - ahead - 1))[i])
        settle(away.at[some], away_in.at[i])
        settle(away.at[some], own_in.at[i])

    def turn():
        raw_load.wait()
        for q in range(nz):
            vectors[q, panel_at(band, slab), :] = raw[pl.ds(q * deep, deep), :].T

    def weigh():
        seats_load.wait()
        for group in range(8):
            row = seats[pl.ds(pl.multiple_of(8 * end, 8), 8), :][group : group + 1, :]
            weight[pl.ds(group * LANES, LANES), :] = jnp.broadcast_to(row, (LANES, LANES)).T

    part[...] = jnp.zeros(part.shape, part.dtype)

    first_steps = pl.ds(0, ahead)

    def sum_to_mate():
        return send(part.at[first_steps], parts.at[0, first_steps], sum_out.at[0], sum_in.at[0], at(mate))

    def sum_to_peer():
        return send(part, parts.at[1], sum_out.at[0], sum_in.at[1], at(peer))

    def total_to(b, i):
        return send(halves.at[x], halves.at[x], sum_out.at[1], sum_in.at[i], at(b))

    @pl.when(inner)
    def _():
        def onward(step, b):
            block(step, b, peer_out, peer, 2).start()

        def share(step, b):
            if isinstance(step, int) and step < ahead:
                block(step, b, share_out, mate, 1).start()

        def mine(step):
            onward(step, band)
            share(step, band)

        def side(step):
            arrived(step, (beside,), 0)
            onward(step, beside)
            share(step, beside)

        def mates(step, which=(0, 1)):
            bands = [(mate, mate_beside)[i] for i in which]
            arrived(step, bands, 1)
            for b in bands:
                onward(step, b)

        def fars(step, which=(0, 1, 2, 3)):
            bands = [(peer, peer_beside, far, far_beside)[i] for i in which]
            arrived(step, bands, 2)
            for b in bands:
                share(step, b)

        def mate_panel(q):
            panel_wait(mate, q)
            panel(mate, q, vec_side, beside).start()
            to_core(mate, q).start()

        loaded(0)
        for step in range(ahead):
            mine(step)
            exchange(step)
        exchange(ahead)
        lax.fori_loop(ahead + 1, steps, load, 0)
        turn()
        for q in range(nz):
            to_core(band, q).start()
        loaded(1)
        for step in range(4, 8):
            exchange(step)
        panel(band, 0, vec_side, beside).start()
        weigh()
        for step in range(ahead):
            side(step)
            mates(step, (0,))
            fars(step, (0,))
        mine(3)
        for step in range(ahead):
            mates(step, (1,))
            fars(step, (1,))
        side(3)
        mates(3)
        mine(4)
        side(4)
        fars(0, (2, 3))
        mate_panel(0)
        fars(1, (2, 3))
        mate_panel(1)
        mine(5)
        fars(2, (2, 3))
        mate_panel(2)
        mate_panel(3)

        def for_mate(step):
            first = (step == ahead).astype(jnp.int32)
            for turn_of in range(2):
                slot = first * (1 - turn_of) + (1 - first) * turn_of
                b = 2 * mate_z + slot * x + (1 - slot) * (1 - x)

                @pl.when(step == ahead)
                def _():
                    if turn_of == 1:
                        mates(step + 1)
                        side(step + 2)
                        mine(step + 3)
                        side(step + 3)
                        for q in range(nz):
                            panel_wait(mate_beside, q)
                            to_core(mate_beside, q).start()
                    core_wait((mate, mate_beside)[turn_of])
                    if turn_of == 1:
                        exchange(step + 5)
                        for q in range(1, nz):
                            panel(band, q, vec_side, beside).start()

                staged[step, slot] = product(step, b)

                @pl.when(slot == 0)
                def _():
                    for p in range(2):
                        to_pass(step, p).start()

                    @pl.when(step == steps - 1)
                    def _():
                        for p in range(2):
                            to_mate_out(step - 1, p).start()

                @pl.when((slot == 1) & (step < steps - 2))
                def _():
                    for p in range(2):
                        to_mate_out(step, p).start()

        def for_row(step, carry):
            staged[step, 2] = product(step, beside)
            for p in range(2):
                to_side_out(staged.at[step, 2, tile(p)], step, p).start()
            staged[step, 3] = product(step, band)
            keep(step).start()
            return carry

        lag = ahead + 3

        def rows_done(step):
            return jnp.minimum(jnp.maximum(step + 1 - lag, 0) * 5 // 3, steps)

        def body(step, carry):
            fars(step)
            for_mate(step)

            @pl.when(step + 2 < steps)
            def _():
                mates(step + 2)

            @pl.when((step > ahead) & (step + 3 < steps))
            def _():
                mine(step + 3)
                side(step + 3)

            @pl.when((step > ahead) & (step + 5 < steps))
            def _():
                exchange(step + 5)

            @pl.when(step == lag)
            def _():
                for q in range(nz):
                    panel_wait(beside, q)
                    to_core(beside, q).start()
                core_wait(band)
                core_wait(beside)

            lax.fori_loop(rows_done(step - 1), rows_done(step), for_row, 0)
            return carry

        lax.fori_loop(ahead, steps, body, 0)
        settle(parts.at[0, first_steps], sum_in.at[0])
        part[first_steps] = part[first_steps] + parts[0, first_steps]
        sum_to_peer().start()
        settle(parts.at[1], sum_in.at[1])
        halves[x] = (part[...] + parts[1]) / jnp.float32(total_bands)
        total_to(mate_beside, 3).start()
        total_to(mate, 2).start()
        total_to(beside, 3).start()
        for p in range(2):
            to_mate_out(steps - 1, p).start()

    @pl.when(outer)
    def _():
        def mine(step):
            block(step, band, mate_out, mate, 1).start()

        def side(step):
            arrived(step, (beside,), 0)
            block(step, beside, mate_out, mate, 1).start()

        loaded(0)
        for step in range(ahead + 1):
            exchange(step)
            mine(step)
        lax.fori_loop(ahead + 1, steps, load, 0)
        turn()
        loaded(1)
        for step in range(ahead + 1, ahead + 5):
            exchange(step)
        for step in range(ahead + 1):
            side(step)
        for q in range(nz):
            panel(band, q, vec_mate, mate).start()
        for q in range(nz):
            panel(band, q, vec_side, beside).start()
            to_core(band, q).start()

        def begin(step, carry):
            exchange(step)
            return carry

        lax.fori_loop(ahead + 5, steps, begin, 0)
        weigh()
        for step in range(ahead + 1, ahead + 5):
            mine(step)
            side(step)
        for q in range(nz):
            panel_wait(beside, q)
            to_core(beside, q).start()
        core_wait(band)
        core_wait(beside)

        def shared(step, carry):
            for b in (mate, mate_beside, peer, peer_beside, far, far_beside):
                settle(gathered.at[step, b], early.at[step, b])
            staged[step, 2] = product(step, beside)
            for p in range(2):
                to_side_out(staged.at[step, 2, tile(p)], step, p).start()
            staged[step, 3] = product(step, band)
            keep(step).start()
            return carry

        lax.fori_loop(0, ahead, shared, 0)
        sum_to_mate().start()

        def body(step, carry):
            @pl.when(step + 5 < steps)
            def _():
                mine(step + 5)
                side(step + 5)

            settle(passing.at[step], pass_in.at[step - ahead])
            for p in range(2):
                to_side_out(passing.at[step, tile(p)], step, p).start()
            return carry

        lax.fori_loop(ahead, steps - 1, body, 0)
        for p in range(2):
            settle(passing.at[steps - 1, tile(p)], pass_in.at[steps - 1 - ahead + p])
            to_side_out(passing.at[steps - 1, tile(p)], steps - 1, p).start()

    @pl.when(outer)
    def _():
        settle(halves.at[x], sum_in.at[2])

    settle(halves.at[1 - x], sum_in.at[3])
    density_copy = pltpu.make_async_copy(halves, density, seats_in.at[0])
    density_copy.start()

    def blocks(n):
        return staged.at[pl.ds(0, n // 2), 0]

    settle(away, away_out.at[0])

    @pl.when(inner)
    def _():
        settle(gathered.at[pl.ds(0, steps // 2)], peer_out.at[0])
        settle(part, sum_out.at[0])
        settle(parts, sum_out.at[1])
        settle(blocks(6 * ahead), share_out.at[0])
        settle(vectors.at[:, pl.ds(0, 4 * width)], vec_core.at[0])
        settle(vectors.at[:, pl.ds(0, 2 * width)], vec_side.at[0])
        settle(staged.at[pl.ds(ahead, steps - ahead), pl.ds(0, 2)], res_mate.at[0])
        settle(blocks(2 * steps), kept.at[0])

    @pl.when(outer)
    def _():
        settle(part.at[first_steps], sum_out.at[0])
        settle(blocks(2 * steps), mate_out.at[0])
        settle(vectors.at[:, pl.ds(0, 2 * width)], vec_core.at[0])
        settle(vectors.at[:, pl.ds(0, width)], vec_side.at[0])
        settle(vectors.at[:, pl.ds(0, width)], vec_mate.at[0])
        settle(blocks(2 * ahead), kept.at[0])
        settle(blocks(2 * (steps - ahead)), mate_in.at[0])

    settle(blocks(2 * steps), side_out.at[0])
    settle(blocks(2 * steps), side_in.at[0])
    density_copy.wait()


def flush(rotated, density, rotated_out, density_out, sems):
    band = rotated.shape[0] // PIECES
    copies = [
        pltpu.make_async_copy(rotated.at[pl.ds(i * band, band)], rotated_out.at[pl.ds(i * band, band)], sems.at[i])
        for i in range(PIECES)
    ]
    copies.append(pltpu.make_async_copy(density, density_out, sems.at[PIECES]))
    for copy in copies:
        copy.start()
    for copy in copies:
        copy.wait()


def local(nb, wavefunctions, eigvec, occupation):
    rows, points = wavefunctions.shape
    total_bands, width = eigvec.shape
    steps = points // 2 // LANES
    if nb != 8 or width != LANES or rows != 2 * width or points % (2 * LANES) or steps < SHARED + 8 or total_bands != nb * rows:
        return plain(wavefunctions, eigvec, occupation)
    nz, deep = nb // 2, total_bands // (nb // 2)
    hbm = pl.BlockSpec(memory_space=pltpu.HBM)
    dma = pltpu.SemaphoreType.DMA
    rotated, density = pl.pallas_call(
        kernel,
        out_shape=(
            pltpu.VMEM((rows, points), jnp.float32),
            pltpu.VMEM((2, steps, 1, LANES), jnp.float32),
        ),
        in_specs=[hbm] * 3,
        out_specs=[pl.BlockSpec(memory_space=pl.ANY)] * 2,
        scratch_shapes=[
            pltpu.VMEM((steps, nb, rows, LANES), jnp.bfloat16),
            pltpu.VMEM((steps, rows, LANES), jnp.bfloat16),
            pltpu.VMEM((total_bands, width), jnp.bfloat16),
            pltpu.VMEM((nz, 4 * rows, deep), jnp.bfloat16),
            pltpu.VMEM((total_bands // LANES, LANES), jnp.float32),
            pltpu.VMEM((4 * rows, LANES), jnp.float32),
            pltpu.VMEM((steps, 4, rows, LANES), jnp.float32),
            pltpu.VMEM((steps, rows, LANES), jnp.float32),
            pltpu.VMEM((steps, 1, LANES), jnp.float32),
            pltpu.VMEM((3, steps, 1, LANES), jnp.float32),
            pltpu.VMEM((2, steps, 1, LANES), jnp.float32),
            dma((2,)),
            dma((2,)),
            dma((1,)),
            dma((1,)),
            dma((SHARED, nb)),
            dma((steps - SHARED, 3)),
            *[dma((1,))] * 4,
            dma((4, nz)),
            dma((4,)),
            *[dma((1,))] * 4,
            dma((steps - SHARED + 1,)),
            *[dma((1,))] * 4,
            dma((2,)),
            dma((4,)),
        ],
        compiler_params=pltpu.CompilerParams(
            collective_id=0, has_side_effects=True, vmem_limit_bytes=56 * 2**20
        ),
    )(wavefunctions, eigvec, occupation.reshape(total_bands // LANES, LANES))
    rotated, density = pl.pallas_call(
        flush,
        out_shape=(
            jax.ShapeDtypeStruct(rotated.shape, rotated.dtype),
            jax.ShapeDtypeStruct(density.shape, density.dtype),
        ),
        in_specs=[pl.BlockSpec(memory_space=pl.ANY)] * 2,
        out_specs=(hbm, hbm),
        scratch_shapes=[dma((PIECES + 1,))],
        compiler_params=pltpu.CompilerParams(vmem_limit_bytes=2**20),
    )(rotated, density)
    return (rotated, density.reshape(points))


def solution(mesh):
    placed = (P("band", ("frag", "slab")), P(None, ("frag", "band", "slab")), P("frag"))
    return jax.shard_map(
        functools.partial(local, mesh.shape["band"]),
        mesh=mesh,
        in_specs=placed,
        out_specs=(P("band", ("frag", "slab")), P(("frag", "slab"))),
        check_vma=False,
    )
```
